32 devices in a mesh: nodes: 32 (over z, y, x, core).
Axes of the slice: x: 2, y: 2, z: 4, core: 2. Of those that a mesh axis runs over, the one named last changes fastest.
Arguments:
- adjacency: bfloat16 [16384, 16384], P('nodes')
- features: bfloat16 [16384, 128], P('nodes')
- w_one: float32 [128, 128], replicated
- w_two: float32 [128, 40], replicated
- labels: int32 [16384], P('nodes')
- label_mask: int32 [16384], P('nodes')
Outputs:
- output 1: float32 [1], replicated
- output 2: float32 [128, 128], replicated
- output 3: float32 [128, 40], replicated
All inputs are finite; a program needn't handle non-finite values.
Results may differ from the reference program's by a relative error of at most 0.001.
Values are sent between devices in bfloat16 or wider.
A program may use at most 1 GiB of HBM per device.

```python
import math
import jax
import jax.numpy as jnp
from jax import lax

NODES = 16384
BLOCK_ROWS = 512
F_IN = 128
HIDDEN = 128
CLASSES = 40

ROW_CONTRACT = (((0,), (0,)), ((), ()))
COL_CONTRACT = (((1,), (1,)), ((), ()))


def setup_inputs(seed: int = 0) -> dict:
    key_list = jax.random.split(jax.random.key(seed), 8)
    num_comms = NODES // BLOCK_ROWS
    shifts = jax.random.randint(key_list[0], (2,), 1, num_comms)
    col_ids = jnp.arange(NODES)
    col_comm = col_ids // BLOCK_ROWS
    row_ids = jnp.arange(BLOCK_ROWS)

    def draw_rows(block_idx):
        hot_cols = (col_comm == (block_idx + shifts[0]) % num_comms) | (col_comm == (block_idx + shifts[1]) % num_comms)
        edge_prob = jnp.where(hot_cols, 0.5, 0.01)
        coin_flip = jax.random.uniform(jax.random.fold_in(key_list[1], block_idx), (BLOCK_ROWS, NODES))
        self_loop = col_ids[None, :] == block_idx * BLOCK_ROWS + row_ids[:, None]
        raw_edges = jnp.where((coin_flip < edge_prob[None, :]) | self_loop, 1.0, 0.0)
        return (raw_edges / jnp.sum(raw_edges, axis=1, keepdims=True)).astype(jnp.bfloat16)

    adjacency = lax.map(draw_rows, jnp.arange(num_comms)).reshape(NODES, NODES)
    centers = jax.random.normal(key_list[2], (num_comms, F_IN))
    feat_noise = jax.random.normal(key_list[3], (NODES, F_IN))
    features = (jnp.repeat(centers, BLOCK_ROWS, axis=0) + feat_noise).astype(jnp.bfloat16)
    w_one = jax.random.normal(key_list[4], (F_IN, HIDDEN)) * math.sqrt(2.0 / F_IN)
    w_two = jax.random.normal(key_list[5], (HIDDEN, CLASSES)) * (2.0 / math.sqrt(HIDDEN))
    labels = jax.random.randint(key_list[6], (NODES,), 0, CLASSES, dtype=jnp.int32)
    drawn_mask = jax.random.randint(key_list[7], (NODES,), 0, 10, dtype=jnp.int32) < 3
    label_mask = jnp.where((jnp.arange(NODES) % 10 == 0) | drawn_mask, 1, 0).astype(jnp.int32)
    return {'adjacency': adjacency, 'features': features, 'w_one': w_one.astype(jnp.float32), 'w_two': w_two.astype(jnp.float32), 'labels': labels, 'label_mask': label_mask}


def reference(adjacency, features, w_one, w_two, labels, label_mask):
    weight_one = w_one.astype(jnp.bfloat16)
    weight_two = w_two.astype(jnp.bfloat16)
    agg_one = jnp.dot(adjacency, features, preferred_element_type=jnp.float32).astype(jnp.bfloat16)
    pre_one = jnp.dot(agg_one, weight_one, preferred_element_type=jnp.float32)
    hidden = jnp.maximum(pre_one, 0.0).astype(jnp.bfloat16)
    agg_two = jnp.dot(adjacency, hidden, preferred_element_type=jnp.float32).astype(jnp.bfloat16)
    logits = jnp.dot(agg_two, weight_two, preferred_element_type=jnp.float32)
    weight = label_mask.astype(jnp.float32)
    label_count = jnp.sum(weight)
    onehot = (labels[:, None] == jnp.arange(CLASSES)[None, :]).astype(jnp.float32)
    log_prob = jax.nn.log_softmax(logits, axis=-1)
    loss_value = -jnp.sum(weight * jnp.sum(onehot * log_prob, axis=-1)) / label_count
    grad_two = (weight[:, None] * (jnp.exp(log_prob) - onehot) / label_count).astype(jnp.bfloat16)
    dw_two = lax.dot_general(agg_two, grad_two, ROW_CONTRACT, preferred_element_type=jnp.float32)
    back_two = lax.dot_general(grad_two, weight_two, COL_CONTRACT, preferred_element_type=jnp.float32).astype(jnp.bfloat16)
    d_hidden = lax.dot_general(adjacency, back_two, ROW_CONTRACT, preferred_element_type=jnp.float32)
    grad_one = jnp.where(pre_one > 0.0, d_hidden, 0.0).astype(jnp.bfloat16)
    dw_one = lax.dot_general(agg_one, grad_one, ROW_CONTRACT, preferred_element_type=jnp.float32)
    return (loss_value.reshape(1), dw_one, dw_two)
```

```python
import functools

import jax
import jax.numpy as jnp
from jax import lax
from jax.experimental import pallas as pl
from jax.experimental.pallas import tpu as pltpu
from jax.sharding import PartitionSpec as P

MESH = pl.DeviceIdType.MESH
F32 = jnp.float32
BF16 = jnp.bfloat16
NDEV = 32
HALVES = 2
F = 128
K = 40
KP = 48
TAIL = 16

STEPS = [[(q, t - (q + 1) // 2) for q in range(4) if 0 <= t - (q + 1) // 2 < 4] for t in range(6)]


def kernel(axis, rows, a_hbm, x_hbm, w1_ref, w2_ref, lab_ref, mask_ref, loss_out, dw1_out, dw2_out,
           a_v, xall, hall, acc, s1, s1t, z1t, w2p, ut, mrow, sq,
           own, outbox, pairin, xin, yin, zin, sums,
           ar1_src, ar1_pin, ar1_pl, ar1_zz, ar1_fin, ar2_src, ar2_pin, ar2_pl, ar2_zz, ar2_fin,
           a_sem, x_sem, ag1_r, ag1_s, ag2_r, ag2_s, rs_ps, rs_pr, rs_xs, rs_xr, rs_ys, rs_yr, rs_zs, rs_zr,
           ar1_s, ar1_r, ar2_s, ar2_r):
    me = lax.axis_index(axis)
    core = me % 2
    x = (me // 2) % 2
    y = (me // 4) % 2
    z = me // 8
    mid = ((z + 1) // 2) % 2
    half = z // 2
    z_in = 1 + z % 2
    z_out = (3 * z - 3) * mid + z * (1 - mid)

    def dev(xx, yy, zz, cc):
        return ((zz * 2 + yy) * 2 + xx) * 2 + cc

    xn, yn = dev(1 - x, y, z, core), dev(x, 1 - y, z, core)
    dn, pn = dev(1 - x, 1 - y, z, core), dev(x, y, z, 1 - core)
    zin_n, zout_n = dev(x, y, z_in, core), dev(x, y, z_out, core)
    zothers = [dev(x, y, (z + k) % 4, core) for k in (1, 2, 3)]

    def zk(j):
        late = j // 2
        line = late * j + (1 - late) * (j + mid * (1 - 2 * j))
        return line + half * (3 - 2 * line)

    def bid(q, j, other=0):
        qx, qy = q % 2, q // 2
        cc = core + other * (1 - 2 * core)
        return dev(x + qx * (1 - 2 * x), y + qy * (1 - 2 * y), zk(j), cc)

    def rcopy(src, dst, ssem, rsem, to):
        return pltpu.make_async_remote_copy(src_ref=src, dst_ref=dst, send_sem=ssem, recv_sem=rsem, device_id=(to,),
                                            device_id_type=MESH)

    def a_copy(b):
        cols = pl.ds(pl.multiple_of(b * rows, rows), rows)
        return pltpu.make_async_copy(a_hbm.at[:, cols], a_v.at[b], a_sem.at[b])

    x_copy = pltpu.make_async_copy(x_hbm, xall.at[me, pl.ds(0, rows)], x_sem)
    x_copy.start()
    for t in range(6):
        for q, j in STEPS[t]:
            a_copy(bid(q, j)).start()
            a_copy(bid(q, j, 1)).start()
    barrier = pltpu.get_barrier_semaphore()
    for to in [pn, xn, yn, dn] + zothers:
        pl.semaphore_signal(barrier, inc=1, device_id=(to,), device_id_type=MESH)
    mrow[...] = jnp.zeros_like(mrow)
    mrow[0:rows // 128, :] = mask_ref[...].astype(F32)
    xall[me, rows:rows + TAIL, :] = mrow[...].astype(BF16)
    w2p[...] = jnp.zeros_like(w2p)
    w2p[:, 0:K] = w2_ref[...]
    w1b = w1_ref[...].astype(BF16)
    acc[...] = jnp.zeros_like(acc)
    x_copy.wait()
    pl.semaphore_wait(barrier, 7)

    def gather(buf, cuts, r_sem, s_sem, first):
        pending = []

        def chunk(b, h):
            return buf.at[b, pl.ds(cuts[h], cuts[h + 1] - cuts[h])]

        def send(b, h, to, cond=None):
            k = len(pending)
            c = rcopy(chunk(b, h), chunk(b, h), s_sem.at[k], r_sem.at[b, h], to)
            pending.append((c, cond))
            if cond is None:
                c.start()
            else:
                pl.when(cond)(c.start)

        def wait_recv(b, h):
            rcopy(chunk(b, h), chunk(b, h), s_sem.at[0], r_sem.at[b, h], pn).wait_recv()

        def mul(b):
            if first:
                a_copy(b).wait()
            acc[...] += jnp.dot(a_v[b], buf[b, 0:rows, :], preferred_element_type=F32)

        is_mid = mid == 1

        def forward(q, j, h):
            b = bid(q, j)
            if q == 0:
                if j == 0:
                    send(b, h, zin_n)
                    send(b, h, zout_n, is_mid)
                elif j == 1:
                    send(b, h, zin_n, is_mid)
                else:
                    send(b, h, zout_n, is_mid)
                send(b, h, xn)
                send(b, h, yn)
            elif q == 1 and j % 2 == 1:
                send(b, h, yn)
            elif q == 2 and j % 2 == 0:
                send(b, h, xn)
            send(b, h, pn)

        def mul_loop(t, other):
            qs = [q for q, _ in STEPS[t]]

            def body(q, carry):
                b = bid(q, t - (q + 1) // 2, other)
                if other:
                    for h in range(HALVES):
                        wait_recv(b, h)
                mul(b)
                return carry
            lax.fori_loop(qs[0], qs[-1] + 1, body, 0)

        for t in range(7):
            if t < 6:
                for h in range(HALVES):
                    for q, j in STEPS[t]:
                        if t > 0:
                            wait_recv(bid(q, j), h)
                        forward(q, j, h)
                mul_loop(t, 0)
            if t > 0:
                mul_loop(t - 1, 1)
        return pending

    def drain(pending):
        for c, cond in pending:
            if cond is None:
                c.wait_send()
            else:
                pl.when(cond)(c.wait_send)

    hr = rows // HALVES
    cuts1 = [h * hr for h in range(HALVES)] + [rows + TAIL]
    cuts2 = [h * hr for h in range(HALVES)] + [rows]
    sends1 = gather(xall, cuts1, ag1_r, ag1_s, True)

    s1b = acc[...].astype(BF16)
    s1[...] = s1b
    z1 = jnp.dot(s1b, w1b, preferred_element_type=F32)
    hall[me] = jnp.maximum(z1, 0.0).astype(BF16)
    sq[...] = z1
    acc[...] = jnp.zeros_like(acc)

    sends2 = gather(hall, cuts2, ag2_r, ag2_s, False)

    w2b = w2p[...].astype(BF16)
    w2t = w2p[...].T[0:KP, :].astype(BF16)

    def count_body(b, tot):
        return tot + xall[b, rows:rows + TAIL, :].astype(F32)
    label_count = jnp.sum(lax.fori_loop(0, NDEV, count_body, jnp.zeros((TAIL, 128), F32)))
    s2b = acc[...].astype(BF16)
    z2 = lax.dot_general(w2t, s2b, (((1,), (1,)), ((), ())), preferred_element_type=F32)
    row_id = lax.broadcasted_iota(jnp.int32, (KP, rows), 0)
    valid = row_id < K
    top = jnp.max(jnp.where(valid, z2, -jnp.inf), axis=0, keepdims=True)
    shifted = jnp.where(valid, z2 - top, 0.0)
    norm = jnp.log(jnp.sum(jnp.where(valid, jnp.exp(shifted), 0.0), axis=0, keepdims=True))
    log_prob = shifted - norm
    hot = row_id == lab_ref[...]
    onehot = jnp.where(hot, 1.0, 0.0)
    weight = jnp.concatenate([mrow[k:k + 1, :] for k in range(rows // 128)], axis=1)
    loss_row = -weight * jnp.sum(jnp.where(hot, log_prob, 0.0), axis=0, keepdims=True)
    g2 = jnp.where(valid, weight * (jnp.exp(log_prob) - onehot) / label_count, 0.0).astype(BF16)
    ut[...] = jnp.dot(w2b[:, 0:KP], g2, preferred_element_type=F32).astype(BF16)
    dw2t = jnp.dot(g2, s2b, preferred_element_type=F32)
    loss_part = loss_row[:, 0:128]
    for k in range(1, rows // 128):
        loss_part = loss_part + loss_row[:, k * 128:(k + 1) * 128]
    ar2_src[...] = dw2t
    ar2_src[K:K + 1, :] = loss_part

    plane = y * 2 + x

    def make_ar(src, pin, pl4, zz, fin, s_sem, r_sem):
        n = src.shape[0] // 2
        sends = []

        def go(c):
            c.start()
            sends.append(c)

        def s1():
            lo = pl.multiple_of((1 - core) * n, n)
            go(rcopy(src.at[pl.ds(lo, n)], pin, s_sem.at[0], r_sem.at[0], pn))

        def s2():
            rcopy(pin, pin, s_sem.at[0], r_sem.at[0], pn).wait_recv()
            lo = pl.multiple_of(core * n, n)
            pl4[plane] = src[pl.ds(lo, n), :] + pin[...]
            for k, to in enumerate((xn, yn, dn)):
                go(rcopy(pl4.at[plane], pl4.at[plane], s_sem.at[1 + k], r_sem.at[1 + plane], to))

        def s3():
            for px, py in ((1, 0), (0, 1), (1, 1)):
                p = (y + py * (1 - 2 * y)) * 2 + x + px * (1 - 2 * x)
                rcopy(pl4.at[p], pl4.at[p], s_sem.at[0], r_sem.at[1 + p], pn).wait_recv()
            zz[z] = (pl4[0] + pl4[1]) + (pl4[2] + pl4[3])
            for k, to in enumerate(zothers):
                go(rcopy(zz.at[z], zz.at[z], s_sem.at[4 + k], r_sem.at[5 + z], to))

        def s4():
            for k in (1, 2, 3):
                o = (z + k) % 4
                rcopy(zz.at[o], zz.at[o], s_sem.at[0], r_sem.at[5 + o], pn).wait_recv()
            fin[core] = (zz[0] + zz[1]) + (zz[2] + zz[3])
            go(rcopy(fin.at[core], fin.at[core], s_sem.at[7], r_sem.at[9], pn))

        def s5():
            rcopy(fin.at[1 - core], fin.at[1 - core], s_sem.at[0], r_sem.at[9], pn).wait_recv()
            for c in sends:
                c.wait_send()

        return s1, s2, s3, s4, s5

    small = make_ar(ar2_src, ar2_pin, ar2_pl, ar2_zz, ar2_fin, ar2_s, ar2_r)
    small[0]()

    def parts(q, j):
        i = q * 4 + j
        outbox[i] = jnp.dot(ut[...], a_v[bid(q, j, 1)], preferred_element_type=F32)
        rcopy(outbox.at[i], pairin.at[i], rs_ps.at[i], rs_pr.at[i], pn).start()
        own[i] = jnp.dot(ut[...], a_v[bid(q, j)], preferred_element_type=F32)

    def diag_body(k, carry):
        parts(3, 3 - k)
        return carry

    def side_body(k, carry):
        parts(1 + k % 2, 3 - k // 2)
        return carry

    def own_body(k, carry):
        parts(0, 3 - k)
        return carry

    fh = F // HALVES

    def hs(h):
        return pl.ds(h * fh, fh)

    def pair_add(q, j):
        i = q * 4 + j
        rcopy(pairin.at[i], pairin.at[i], rs_ps.at[0], rs_pr.at[i], pn).wait_recv()
        own[i] = own[i] + pairin[i]

    def xslot(q, j):
        return 2 + j if q == 0 else (3 - j) // 2

    rs_sends = []

    def rs_send(src, dst, s_arr, r_arr, k, h, dk, to):
        c = rcopy(src, dst, s_arr.at[k, h], r_arr.at[dk, h], to)
        c.start()
        rs_sends.append(c)

    lax.fori_loop(0, 4, diag_body, 0)
    for j in (3, 2, 1, 0):
        pair_add(3, j)
        for h in range(HALVES):
            if j % 2 == 1:
                s = xslot(2, j)
                rs_send(own.at[12 + j, hs(h)], xin.at[s, hs(h)], rs_xs, rs_xr, s, h, s, xn)
            else:
                s = xslot(1, j)
                rs_send(own.at[12 + j, hs(h)], yin.at[s, hs(h)], rs_ys, rs_yr, s, h, s, yn)
    lax.fori_loop(0, 8, side_body, 0)
    small[1]()
    lax.fori_loop(0, 4, own_body, 0)
    for j in (3, 2, 1, 0):
        pair_add(1, j)
        pair_add(2, j)
    for j in (3, 2, 1, 0):
        for h in range(HALVES):
            ix, iy = 4 + j, 8 + j
            if j % 2 == 1:
                s = xslot(2, j)
                rcopy(xin.at[s, hs(h)], xin.at[s, hs(h)], rs_xs.at[0, 0], rs_xr.at[s, h], pn).wait_recv()
                own[iy, hs(h)] = own[iy, hs(h)] + xin[s, hs(h)]
            else:
                s = xslot(1, j)
                rcopy(yin.at[s, hs(h)], yin.at[s, hs(h)], rs_ys.at[0, 0], rs_yr.at[s, h], pn).wait_recv()
                own[ix, hs(h)] = own[ix, hs(h)] + yin[s, hs(h)]
            rs_send(own.at[ix, hs(h)], xin.at[2 + j, hs(h)], rs_xs, rs_xr, 2 + j, h, 2 + j, xn)
            rs_send(own.at[iy, hs(h)], yin.at[2 + j, hs(h)], rs_ys, rs_yr, 2 + j, h, 2 + j, yn)
    for j in (3, 2, 1, 0):
        pair_add(0, j)
    small[2]()

    z1t[...] = sq[...].T
    s1t[...] = s1[...].astype(F32).T.astype(BF16)

    def z_wait(s, h):
        rcopy(zin.at[s, hs(h)], zin.at[s, hs(h)], rs_zs.at[0, 0], rs_zr.at[s, h], pn).wait_recv()

    for j in (3, 2, 1, 0):
        for h in range(HALVES):
            for arr, r_arr in ((xin, rs_xr), (yin, rs_yr)):
                rcopy(arr.at[2 + j, hs(h)], arr.at[2 + j, hs(h)], rs_xs.at[0, 0], r_arr.at[2 + j, h], pn).wait_recv()
            sums[j, hs(h)] = (own[j, hs(h)] + xin[2 + j, hs(h)]) + yin[2 + j, hs(h)]

            @pl.when(mid == 1)
            def _():
                s = {3: 3, 2: 2, 1: 5, 0: 0}[j]
                z_wait(s, h)
                sums[j, hs(h)] = sums[j, hs(h)] + zin[s, hs(h)]
            if j > 0:
                to = zin_n if j > 1 else dev(x, y, z_in + mid * (z_out - z_in), core)
                slot = j + 2 * mid if j > 1 else 4 * mid
                rs_send(sums.at[j, hs(h)], zin.at[slot, hs(h)], rs_zs, rs_zr, j, h, slot, to)
            else:
                z_wait(4, h)
                sums[0, hs(h)] = sums[0, hs(h)] + zin[4, hs(h)]
        if j == 3:
            small[3]()

    g1t = jnp.where(z1t[...] > 0.0, sums[0], 0.0).astype(BF16)
    ar1_src[...] = lax.dot_general(s1t[...], g1t, (((1,), (1,)), ((), ())), preferred_element_type=F32)
    big = make_ar(ar1_src, ar1_pin, ar1_pl, ar1_zz, ar1_fin, ar1_s, ar1_r)
    big[0]()
    small[4]()
    w2p[0:KP // 2, :] = ar2_fin[0]
    w2p[KP // 2:KP, :] = ar2_fin[1]
    loss_out[0] = jnp.sum(w2p[K:K + 1, :]) / label_count
    dw2_out[...] = w2p[...].T[:, 0:K]
    big[1]()
    drain(sends1)
    drain(sends2)
    big[2]()
    for c in rs_sends:
        c.wait_send()
    for i in range(16):
        rcopy(outbox.at[i], pairin.at[i], rs_ps.at[i], rs_pr.at[i], pn).wait_send()
    big[3]()
    big[4]()
    dw1_out[0:F // 2, :] = ar1_fin[0]
    dw1_out[F // 2:F, :] = ar1_fin[1]


def solution(mesh):
    axis = 'nodes'

    def local_step(adj_rows, feat_rows, w_one, w_two, label_rows, mask_rows):
        rows = adj_rows.shape[0]
        dma = pltpu.SemaphoreType.DMA
        nsend = 64 * HALVES
        blk = lambda n: pltpu.VMEM((n, F, rows), F32)
        ar = lambda n: [pltpu.VMEM((2 * n, F), F32), pltpu.VMEM((n, F), F32), pltpu.VMEM((4, n, F), F32),
                        pltpu.VMEM((4, n, F), F32), pltpu.VMEM((2, n, F), F32)]
        vmem = pl.BlockSpec(memory_space=pltpu.VMEM)
        hbm = pl.BlockSpec(memory_space=pl.ANY)
        return pl.pallas_call(
            functools.partial(kernel, axis, rows),
            name='gcn_step',
            out_shape=(jax.ShapeDtypeStruct((1,), F32), jax.ShapeDtypeStruct((F, F), F32),
                       jax.ShapeDtypeStruct((F, K), F32)),
            in_specs=[hbm, hbm, vmem, vmem, vmem, vmem],
            out_specs=(pl.BlockSpec(memory_space=pltpu.SMEM), vmem, vmem),
            scratch_shapes=[
                pltpu.VMEM((NDEV, rows, rows), BF16), pltpu.VMEM((NDEV, rows + TAIL, F), BF16),
                pltpu.VMEM((NDEV, rows, F), BF16), pltpu.VMEM((rows, F), F32), pltpu.VMEM((rows, F), BF16),
                pltpu.VMEM((F, rows), BF16), pltpu.VMEM((F, rows), F32), pltpu.VMEM((F, F), F32),
                pltpu.VMEM((F, rows), BF16), pltpu.VMEM((TAIL, F), F32), pltpu.VMEM((rows, F), F32),
                blk(16), blk(16), blk(16), blk(6), blk(6), blk(6), blk(4),
                *ar(F // 2), *ar(KP // 2),
                dma((NDEV,)), dma(()), dma((NDEV, HALVES)), dma((nsend,)), dma((NDEV, HALVES)), dma((nsend,)),
                dma((16,)), dma((16,)), dma((6, HALVES)), dma((6, HALVES)), dma((6, HALVES)), dma((6, HALVES)),
                dma((6, HALVES)), dma((6, HALVES)), dma((8,)), dma((10,)), dma((8,)), dma((10,)),
            ],
            compiler_params=pltpu.CompilerParams(collective_id=0, has_side_effects=True,
                                                 vmem_limit_bytes=60 * 1024 * 1024),
        )(adj_rows, feat_rows, w_one, w_two, label_rows.reshape(1, rows), mask_rows.reshape(rows // 128, 128))

    return jax.shard_map(local_step, mesh=mesh,
                         in_specs=(P(axis, None), P(axis, None), P(None, None), P(None, None), P(axis), P(axis)),
                         out_specs=(P(None), P(None, None), P(None, None)), check_vma=False)
```

```python
import functools

import jax
import jax.numpy as jnp
from jax import lax
from jax.experimental import pallas as pl
from jax.experimental.pallas import tpu as pltpu
from jax.sharding import PartitionSpec as P

MESH = pl.DeviceIdType.MESH
F32 = jnp.float32
BF16 = jnp.bfloat16
NDEV = 32
HALVES = 2
F = 128
K = 40
KP = 48
TAIL = 16

ORDER_END = (
    0, 16, 32, 1, 17, 40, 8, 2, 36, 5, 18, 21, 33, 44, 37, 24, 3, 12, 19, 34, 38, 10, 22, 28,
    29, 13, 26, 4, 7, 9, 6, 45, 23, 43, 41, 42, 11, 20, 39, 27, 25, 15, 30, 14, 46, 35, 47, 31,
)
ORDER_MID = (
    0, 16, 32, 2, 1, 18, 17, 36, 40, 3, 19, 10, 41, 26, 24, 34, 5, 38, 37, 42, 21, 44, 33, 4,
    43, 11, 20, 7, 45, 39, 8, 23, 9, 46, 27, 35, 22, 47, 14, 25, 30, 6, 15, 31, 13, 28, 29, 12,
)
PIECES = 3
BATCH = 4


def program(order):
    seen, steps, ready, late, following = {}, [], [], [], []
    for code in order:
        c, q, j = code // 16, code // 4 % 4, code % 4
        steps.append((c, q, j))
        seen[q, j] = seen.get((q, j), 0) + 1
        if seen[q, j] == PIECES:
            ready.append((q, j))
            following.append((q, j))
            if len(ready) + len(late) >= BATCH:
                steps.append((ready, late))
                ready, late, following = [], following, []
    return steps + [(ready, late), ([], following)]


def kernel(axis, rows, a_hbm, x_hbm, w1_ref, w2_ref, lab_ref, mask_ref, out_ref,
           a_v, xall, hall, acc, s1, s1t, z1t, w2p, ut, mrow, sq,
           own, outbox, pairin, xin, yin, zin, sums,
           ar1_src, ar1_pin, ar1_pl, ar1_zz, ar1_fin, ar2_src, ar2_pin, ar2_pl, ar2_zz, ar2_fin,
           a_sem, x_sem, ag1_r, ag1_s, ag2_r, ag2_s, rs_ps, rs_pr, rs_xs, rs_xr, rs_ys, rs_yr, rs_zs, rs_zr,
           ar1_s, ar1_r, ar2_s, ar2_r):
    me = lax.axis_index(axis)
    core = me % 2
    x = (me // 2) % 2
    y = (me // 4) % 2
    z = me // 8
    mid = ((z + 1) // 2) % 2
    half = z // 2
    z_in = 1 + z % 2
    z_out = (3 * z - 3) * mid + z * (1 - mid)

    def dev(xx, yy, zz, cc):
        return ((zz * 2 + yy) * 2 + xx) * 2 + cc

    xn, yn = dev(1 - x, y, z, core), dev(x, 1 - y, z, core)
    dn, pn = dev(1 - x, 1 - y, z, core), dev(x, y, z, 1 - core)
    zin_n, zout_n = dev(x, y, z_in, core), dev(x, y, z_out, core)
    zothers = [dev(x, y, (z + k) % 4, core) for k in (1, 2, 3)]

    def zk(j):
        late = j // 2
        line = late * j + (1 - late) * (j + mid * (1 - 2 * j))
        return line + half * (3 - 2 * line)

    def bid(q, j, other=0):
        qx, qy = q % 2, q // 2
        cc = core + other * (1 - 2 * core)
        return dev(x + qx * (1 - 2 * x), y + qy * (1 - 2 * y), zk(j), cc)

    def rcopy(src, dst, ssem, rsem, to):
        return pltpu.make_async_remote_copy(src_ref=src, dst_ref=dst, send_sem=ssem, recv_sem=rsem, device_id=(to,),
                                            device_id_type=MESH)

    def a_copy(b):
        cols = pl.ds(pl.multiple_of(b * rows, rows), rows)
        return pltpu.make_async_copy(a_hbm.at[:, cols], a_v.at[b], a_sem.at[b])

    x_copy = pltpu.make_async_copy(x_hbm, xall.at[me, pl.ds(0, rows)], x_sem)
    x_copy.start()
    blocks = {(q, j, o): bid(q, j, o) for q in range(4) for j in range(4) for o in range(2)}
    for b in blocks.values():
        a_copy(b).start()
    barrier = pltpu.get_barrier_semaphore()
    for to in [pn, xn, yn, dn] + zothers:
        pl.semaphore_signal(barrier, inc=1, device_id=(to,), device_id_type=MESH)
    mrow[...] = jnp.zeros_like(mrow)
    mrow[0:rows // 128, :] = mask_ref[...].astype(F32)
    xall[me, rows:rows + TAIL, :] = mrow[...].astype(BF16)
    w2p[...] = jnp.zeros_like(w2p)
    w2p[0:K, :] = w2_ref[...]
    w1b = w1_ref[...].astype(BF16)
    acc[...] = jnp.zeros_like(acc)
    x_copy.wait()
    pl.semaphore_wait(barrier, 7)

    is_mid = mid == 1

    def pick(i, values):
        out = values[0]
        for k in range(1, len(values)):
            out = jnp.where(i == k, values[k], out)
        return out

    def gather(buf, cuts, r_sem, s_sem, first):
        def piece(b, c):
            return buf.at[b, pl.ds(cuts[c], cuts[c + 1] - cuts[c])]

        def wait_recv(b, c):
            rcopy(piece(b, c), piece(b, c), s_sem.at[0], r_sem.at[b, c], pn).wait_recv()

        def targets(c, q, j, between):
            to = []
            if q == 0 or c == 2:
                if j == 0:
                    to += [zin_n, zout_n] if between else [zin_n]
                elif between:
                    to += [zin_n if j == 1 else zout_n]
            if q == 0 and (c < 2 or j == 0):
                to += [xn, yn]
            elif (q == 2 and c < 2 and j % 2 == 0) or (q == 2 and c == 2 and j == 0):
                to += [xn]
            elif q == 1 and c < 2 and j % 2 == 1:
                to += [yn]
            return to + [pn]

        def multiply(ready, late):
            ids = [blocks[q, j, 0] for q, j in ready] + [blocks[q, j, 1] for q, j in late]
            if not ids:
                return

            def body(i, carry):
                b = pick(i, ids)
                if late:
                    @pl.when(i >= len(ready))
                    def _():
                        for c in range(PIECES):
                            wait_recv(b, c)
                if first:
                    a_copy(b).wait()
                acc[...] += jnp.dot(a_v[b], buf[b, 0:rows, :], preferred_element_type=F32)
                return carry
            lax.fori_loop(0, len(ids), body, 0)

        def run(order, between, pending):
            for step in program(order):
                if len(step) == 2:
                    multiply(*step)
                    continue
                c, q, j = step
                b = blocks[q, j, 0]
                if (q, j) != (0, 0):
                    wait_recv(b, c)
                for to in targets(c, q, j, between):
                    k = len(pending)
                    rcopy(piece(b, c), piece(b, c), s_sem.at[k], r_sem.at[b, c], to).start()
                    pending.append((b, c, to))

        sent = {True: [], False: []}

        @pl.when(is_mid)
        def _():
            run(ORDER_MID, True, sent[True])

        @pl.when(mid == 0)
        def _():
            run(ORDER_END, False, sent[False])

        def drain():
            for between, when in ((True, is_mid), (False, mid == 0)):
                @pl.when(when)
                def _():
                    for k, (b, c, to) in enumerate(sent[between]):
                        rcopy(piece(b, c), piece(b, c), s_sem.at[k], r_sem.at[b, c], to).wait_send()
        return drain

    cuts1 = (0, rows * 3 // 8, rows * 6 // 8, rows + TAIL)
    cuts2 = (0, rows * 3 // 8, rows * 6 // 8, rows)
    drain1 = gather(xall, cuts1, ag1_r, ag1_s, True)

    s1b = acc[...].astype(BF16)
    s1[...] = s1b
    z1 = jnp.dot(s1b, w1b, preferred_element_type=F32)
    hall[me] = jnp.maximum(z1, 0.0).astype(BF16)
    sq[...] = z1
    acc[...] = jnp.zeros_like(acc)

    drain2 = gather(hall, cuts2, ag2_r, ag2_s, False)

    w2b = w2p[...].T.astype(BF16)
    w2t = w2p[0:KP, :].astype(BF16)

    def count_body(b, tot):
        return tot + xall[b, rows:rows + TAIL, :].astype(F32)
    label_count = jnp.sum(lax.fori_loop(0, NDEV, count_body, jnp.zeros((TAIL, 128), F32)))
    s2b = acc[...].astype(BF16)
    z2 = lax.dot_general(w2t, s2b, (((1,), (1,)), ((), ())), preferred_element_type=F32)
    row_id = lax.broadcasted_iota(jnp.int32, (KP, rows), 0)
    valid = row_id < K
    top = jnp.max(jnp.where(valid, z2, -jnp.inf), axis=0, keepdims=True)
    shifted = jnp.where(valid, z2 - top, 0.0)
    norm = jnp.log(jnp.sum(jnp.where(valid, jnp.exp(shifted), 0.0), axis=0, keepdims=True))
    log_prob = shifted - norm
    hot = row_id == lab_ref[...]
    onehot = jnp.where(hot, 1.0, 0.0)
    weight = jnp.concatenate([mrow[k:k + 1, :] for k in range(rows // 128)], axis=1)
    loss_row = -weight * jnp.sum(jnp.where(hot, log_prob, 0.0), axis=0, keepdims=True)
    g2 = jnp.where(valid, weight * (jnp.exp(log_prob) - onehot) / label_count, 0.0).astype(BF16)
    ut[...] = jnp.dot(w2b[:, 0:KP], g2, preferred_element_type=F32).astype(BF16)
    dw2t = jnp.dot(g2, s2b, preferred_element_type=F32)
    loss_part = loss_row[:, 0:128]
    for k in range(1, rows // 128):
        loss_part = loss_part + loss_row[:, k * 128:(k + 1) * 128]
    ar2_src[...] = dw2t
    ar2_src[K:K + 1, :] = loss_part

    plane = y * 2 + x

    def make_ar(src, pin, pl4, zz, fin, s_sem, r_sem):
        n = src.shape[0] // 2
        sends = []

        def go(c):
            c.start()
            sends.append(c)

        def s1():
            lo = pl.multiple_of((1 - core) * n, n)
            go(rcopy(src.at[pl.ds(lo, n)], pin, s_sem.at[0], r_sem.at[0], pn))

        def s2():
            rcopy(pin, pin, s_sem.at[0], r_sem.at[0], pn).wait_recv()
            lo = pl.multiple_of(core * n, n)
            pl4[plane] = src[pl.ds(lo, n), :] + pin[...]
            for k, to in enumerate((xn, yn, dn)):
                go(rcopy(pl4.at[plane], pl4.at[plane], s_sem.at[1 + k], r_sem.at[1 + plane], to))

        def s3():
            for px, py in ((1, 0), (0, 1), (1, 1)):
                p = (y + py * (1 - 2 * y)) * 2 + x + px * (1 - 2 * x)
                rcopy(pl4.at[p], pl4.at[p], s_sem.at[0], r_sem.at[1 + p], pn).wait_recv()
            zz[z] = (pl4[0] + pl4[1]) + (pl4[2] + pl4[3])
            for k, to in enumerate(zothers):
                go(rcopy(zz.at[z], zz.at[z], s_sem.at[4 + k], r_sem.at[5 + z], to))

        def s4():
            for k in (1, 2, 3):
                o = (z + k) % 4
                rcopy(zz.at[o], zz.at[o], s_sem.at[0], r_sem.at[5 + o], pn).wait_recv()
            fin[core] = (zz[0] + zz[1]) + (zz[2] + zz[3])
            go(rcopy(fin.at[core], fin.at[core], s_sem.at[7], r_sem.at[9], pn))

        def s5():
            rcopy(fin.at[1 - core], fin.at[1 - core], s_sem.at[0], r_sem.at[9], pn).wait_recv()
            for c in sends:
                c.wait_send()

        return s1, s2, s3, s4, s5

    small = make_ar(ar2_src, ar2_pin, ar2_pl, ar2_zz, ar2_fin, ar2_s, ar2_r)
    small[0]()

    def parts(q, j):
        i = q * 4 + j
        outbox[i] = jnp.dot(ut[...], a_v[bid(q, j, 1)], preferred_element_type=F32)
        rcopy(outbox.at[i], pairin.at[i], rs_ps.at[i], rs_pr.at[i], pn).start()
        own[i] = jnp.dot(ut[...], a_v[bid(q, j)], preferred_element_type=F32)

    def diag_body(k, carry):
        parts(3, 3 - k)
        return carry

    def side_body(k, carry):
        parts(1 + k % 2, 3 - k // 2)
        return carry

    def own_body(k, carry):
        parts(0, 3 - k)
        return carry

    fh = F // HALVES

    def hs(h):
        return pl.ds(h * fh, fh)

    def pair_add(q, j):
        i = q * 4 + j
        rcopy(pairin.at[i], pairin.at[i], rs_ps.at[0], rs_pr.at[i], pn).wait_recv()
        own[i] = own[i] + pairin[i]

    def xslot(q, j):
        return 2 + j if q == 0 else (3 - j) // 2

    rs_sends = []

    def rs_send(src, dst, s_arr, r_arr, k, h, dk, to):
        c = rcopy(src, dst, s_arr.at[k, h], r_arr.at[dk, h], to)
        c.start()
        rs_sends.append(c)

    lax.fori_loop(0, 4, diag_body, 0)
    for j in (3, 2, 1, 0):
        pair_add(3, j)
        for h in range(HALVES):
            if j % 2 == 1:
                s = xslot(2, j)
                rs_send(own.at[12 + j, hs(h)], xin.at[s, hs(h)], rs_xs, rs_xr, s, h, s, xn)
            else:
                s = xslot(1, j)
                rs_send(own.at[12 + j, hs(h)], yin.at[s, hs(h)], rs_ys, rs_yr, s, h, s, yn)
    lax.fori_loop(0, 8, side_body, 0)
    small[1]()
    lax.fori_loop(0, 4, own_body, 0)
    for j in (3, 2, 1, 0):
        pair_add(1, j)
        pair_add(2, j)
    for j in (3, 2, 1, 0):
        for h in range(HALVES):
            ix, iy = 4 + j, 8 + j
            if j % 2 == 1:
                s = xslot(2, j)
                rcopy(xin.at[s, hs(h)], xin.at[s, hs(h)], rs_xs.at[0, 0], rs_xr.at[s, h], pn).wait_recv()
                own[iy, hs(h)] = own[iy, hs(h)] + xin[s, hs(h)]
            else:
                s = xslot(1, j)
                rcopy(yin.at[s, hs(h)], yin.at[s, hs(h)], rs_ys.at[0, 0], rs_yr.at[s, h], pn).wait_recv()
                own[ix, hs(h)] = own[ix, hs(h)] + yin[s, hs(h)]
            rs_send(own.at[ix, hs(h)], xin.at[2 + j, hs(h)], rs_xs, rs_xr, 2 + j, h, 2 + j, xn)
            rs_send(own.at[iy, hs(h)], yin.at[2 + j, hs(h)], rs_ys, rs_yr, 2 + j, h, 2 + j, yn)
    for j in (3, 2, 1, 0):
        pair_add(0, j)
    small[2]()

    z1t[...] = sq[...].T
    s1t[...] = s1[...].astype(F32).T.astype(BF16)

    def z_wait(s, h):
        rcopy(zin.at[s, hs(h)], zin.at[s, hs(h)], rs_zs.at[0, 0], rs_zr.at[s, h], pn).wait_recv()

    for j in (3, 2, 1, 0):
        for h in range(HALVES):
            for arr, r_arr in ((xin, rs_xr), (yin, rs_yr)):
                rcopy(arr.at[2 + j, hs(h)], arr.at[2 + j, hs(h)], rs_xs.at[0, 0], r_arr.at[2 + j, h], pn).wait_recv()
            sums[j, hs(h)] = (own[j, hs(h)] + xin[2 + j, hs(h)]) + yin[2 + j, hs(h)]

            @pl.when(mid == 1)
            def _():
                s = {3: 3, 2: 2, 1: 5, 0: 0}[j]
                z_wait(s, h)
                sums[j, hs(h)] = sums[j, hs(h)] + zin[s, hs(h)]
            if j > 0:
                to = zin_n if j > 1 else dev(x, y, z_in + mid * (z_out - z_in), core)
                slot = j + 2 * mid if j > 1 else 4 * mid
                rs_send(sums.at[j, hs(h)], zin.at[slot, hs(h)], rs_zs, rs_zr, j, h, slot, to)
            else:
                z_wait(4, h)
                sums[0, hs(h)] = sums[0, hs(h)] + zin[4, hs(h)]
        if j == 3:
            small[3]()

    g1t = jnp.where(z1t[...] > 0.0, sums[0], 0.0).astype(BF16)
    ar1_src[...] = lax.dot_general(s1t[...], g1t, (((1,), (1,)), ((), ())), preferred_element_type=F32)
    big = make_ar(ar1_src, ar1_pin, ar1_pl, ar1_zz, ar1_fin, ar1_s, ar1_r)
    big[0]()
    small[4]()
    out_ref[F:F + KP // 2, :] = ar2_fin[0]
    out_ref[F + KP // 2:F + KP, :] = ar2_fin[1]
    loss_row = out_ref[F + K:F + K + 1, :]
    out_ref[F + K:F + K + 1, :] = jnp.sum(loss_row, axis=1, keepdims=True) / label_count + jnp.zeros_like(loss_row)
    big[1]()
    drain1()
    drain2()
    big[2]()
    for c in rs_sends:
        c.wait_send()
    for i in range(16):
        rcopy(outbox.at[i], pairin.at[i], rs_ps.at[i], rs_pr.at[i], pn).wait_send()
    big[3]()
    big[4]()
    out_ref[0:F // 2, :] = ar1_fin[0]
    out_ref[F // 2:F, :] = ar1_fin[1]


def unpack(packed, loss_out, dw1_out, dw2_out):
    loss_out[0] = packed[F + K, 0]
    dw1_out[...] = packed[0:F, :]
    dw2_out[...] = packed[F:F + K, :]


def solution(mesh):
    axis = 'nodes'

    def local_step(adj_rows, feat_rows, w_one, w_two, label_rows, mask_rows):
        rows = adj_rows.shape[0]
        dma = pltpu.SemaphoreType.DMA
        nsend = 144
        blk = lambda n: pltpu.VMEM((n, F, rows), F32)
        ar = lambda n: [pltpu.VMEM((2 * n, F), F32), pltpu.VMEM((n, F), F32), pltpu.VMEM((4, n, F), F32),
                        pltpu.VMEM((4, n, F), F32), pltpu.VMEM((2, n, F), F32)]
        vmem = pl.BlockSpec(memory_space=pltpu.VMEM)
        hbm = pl.BlockSpec(memory_space=pl.ANY)
        packed = pl.pallas_call(
            functools.partial(kernel, axis, rows),
            name='gcn_step',
            out_shape=jax.ShapeDtypeStruct((F + KP, F), F32),
            in_specs=[hbm, hbm, vmem, vmem, vmem, vmem],
            out_specs=vmem,
            scratch_shapes=[
                pltpu.VMEM((NDEV, rows, rows), BF16), pltpu.VMEM((NDEV, rows + TAIL, F), BF16),
                pltpu.VMEM((NDEV, rows, F), BF16), pltpu.VMEM((rows, F), F32), pltpu.VMEM((rows, F), BF16),
                pltpu.VMEM((F, rows), BF16), pltpu.VMEM((F, rows), F32), pltpu.VMEM((F, F), F32),
                pltpu.VMEM((F, rows), BF16), pltpu.VMEM((TAIL, F), F32), pltpu.VMEM((rows, F), F32),
                blk(16), blk(16), blk(16), blk(6), blk(6), blk(6), blk(4),
                *ar(F // 2), *ar(KP // 2),
                dma((NDEV,)), dma(()), dma((NDEV, PIECES)), dma((nsend,)), dma((NDEV, PIECES)), dma((nsend,)),
                dma((16,)), dma((16,)), dma((6, HALVES)), dma((6, HALVES)), dma((6, HALVES)), dma((6, HALVES)),
                dma((6, HALVES)), dma((6, HALVES)), dma((8,)), dma((10,)), dma((8,)), dma((10,)),
            ],
            compiler_params=pltpu.CompilerParams(collective_id=0, has_side_effects=True,
                                                 vmem_limit_bytes=60 * 1024 * 1024),
        )(adj_rows, feat_rows, w_one, w_two.T, label_rows.reshape(1, rows), mask_rows.reshape(rows // 128, 128))
        loss, dw_one, dw_two_t = pl.pallas_call(
            unpack,
            name='unpack',
            out_shape=(jax.ShapeDtypeStruct((1,), F32), jax.ShapeDtypeStruct((F, F), F32),
                       jax.ShapeDtypeStruct((K, F), F32)),
            in_specs=[vmem],
            out_specs=(pl.BlockSpec(memory_space=pltpu.SMEM), vmem, vmem),
        )(packed)
        return loss, dw_one, dw_two_t.T

    return jax.shard_map(local_step, mesh=mesh,
                         in_specs=(P(axis, None), P(axis, None), P(None, None), P(None, None), P(axis), P(axis)),
                         out_specs=(P(None), P(None, None), P(None, None)), check_vma=False)
```

```python
import functools

import jax
import jax.numpy as jnp
from jax import lax
from jax.experimental import pallas as pl
from jax.experimental.pallas import tpu as pltpu
from jax.sharding import PartitionSpec as P

MESH = pl.DeviceIdType.MESH
F32 = jnp.float32
BF16 = jnp.bfloat16
NDEV = 32
F = 128
K = 40
KP = 48
TAIL = 16

ORDER_END = (
    0, 16, 32, 1, 17, 40, 8, 2, 36, 5, 18, 21, 33, 44, 37, 24, 3, 12, 19, 34, 38, 10, 22, 28,
    29, 13, 26, 4, 7, 9, 6, 45, 23, 43, 41, 42, 11, 20, 39, 27, 25, 15, 30, 14, 46, 35, 47, 31,
)
ORDER_MID = (
    0, 16, 32, 2, 1, 18, 17, 36, 40, 3, 19, 10, 41, 26, 24, 34, 5, 38, 37, 42, 21, 44, 33, 4,
    43, 11, 20, 7, 45, 39, 8, 23, 9, 46, 27, 35, 22, 47, 14, 25, 30, 6, 15, 31, 13, 28, 29, 12,
)
PIECES = 3
BATCH = 4

CALC, DIAG, XSIDE, YSIDE, LINE, BACK, BDIAG, BX, BY, BEND = range(10)
CUTS = (0, 48, 96, 128)
REDUCE_END = (
    1, 367, 83, 66, 365, 366, 67, 81, 82, 2, 147, 359, 65, 211, 130, 210, 131, 145, 363, 3, 362, 64, 355, 146,
    358, 80, 354, 195, 364, 275, 194, 357, 208, 361, 356, 193, 416, 129, 144, 209, 259, 258, 192, 480, 360, 274, 353, 128,
    352, 544, 257, 273, 608, 272, 256,
)
REDUCE_MID = (
    1, 83, 82, 81, 80, 64, 66, 67, 2, 367, 211, 65, 209, 366, 365, 147, 359, 363, 144, 3, 362, 355, 193, 145,
    357, 361, 130, 195, 354, 358, 194, 131, 210, 364, 416, 208, 353, 275, 356, 129, 146, 480, 259, 273, 192, 258, 360, 257,
    128, 544, 274, 256, 352, 608, 272,
)


def program(order):
    seen, steps, ready, late, following = {}, [], [], [], []
    for code in order:
        c, q, j = code // 16, code // 4 % 4, code % 4
        steps.append((c, q, j))
        seen[q, j] = seen.get((q, j), 0) + 1
        if seen[q, j] == PIECES:
            ready.append((q, j))
            following.append((q, j))
            if len(ready) + len(late) >= BATCH:
                steps.append((ready, late))
                ready, late, following = [], following, []
    return steps + [(ready, late), ([], following)]


def kernel(axis, rows, a_hbm, x_hbm, w1_ref, w2_ref, lab_ref, mask_ref, out_ref,
           a_v, xall, hall, acc, s1, s1t, z1t, w2p, w2b, ut, mrow, cnt, sq,
           own, outbox, pairin, xin, yin, zin, zinb,
           ar1_src, ar1_pin, ar1_pl, ar1_zz, ar1_fin, ar2_src, ar2_pin, ar2_pl, ar2_zz, ar2_fin,
           a_sem, x_sem, ag1_r, ag1_s, ag2_r, ag2_s, rs_ps, rs_pr, rs_s, rs_xr, rs_yr, rs_zr, rs_br,
           ar1_s, ar1_r, ar2_s, ar2_r):
    me = lax.axis_index(axis)
    core = me % 2
    x = (me // 2) % 2
    y = (me // 4) % 2
    z = me // 8
    mid = ((z + 1) // 2) % 2
    half = z // 2
    z_in = 1 + z % 2
    z_out = (3 * z - 3) * mid + z * (1 - mid)

    def dev(xx, yy, zz, cc):
        return ((zz * 2 + yy) * 2 + xx) * 2 + cc

    xn, yn = dev(1 - x, y, z, core), dev(x, 1 - y, z, core)
    dn, pn = dev(1 - x, 1 - y, z, core), dev(x, y, z, 1 - core)
    zin_n, zout_n = dev(x, y, z_in, core), dev(x, y, z_out, core)
    zothers = [dev(x, y, (z + k) % 4, core) for k in (1, 2, 3)]

    def zk(j):
        late = j // 2
        line = late * j + (1 - late) * (j + mid * (1 - 2 * j))
        return line + half * (3 - 2 * line)

    def bid(q, j, other=0):
        qx, qy = q % 2, q // 2
        cc = core + other * (1 - 2 * core)
        return dev(x + qx * (1 - 2 * x), y + qy * (1 - 2 * y), zk(j), cc)

    def rcopy(src, dst, ssem, rsem, to):
        return pltpu.make_async_remote_copy(src_ref=src, dst_ref=dst, send_sem=ssem, recv_sem=rsem, device_id=(to,),
                                            device_id_type=MESH)

    def a_copy(b):
        cols = pl.ds(pl.multiple_of(b * rows, rows), rows)
        return pltpu.make_async_copy(a_hbm.at[:, cols], a_v.at[b], a_sem.at[b])

    x_copy = pltpu.make_async_copy(x_hbm, xall.at[me, pl.ds(0, rows)], x_sem)
    x_copy.start()
    blocks = {(q, j, o): bid(q, j, o) for q in range(4) for j in range(4) for o in range(2)}
    for b in blocks.values():
        a_copy(b).start()
    barrier = pltpu.get_barrier_semaphore()
    for to in [pn, xn, yn, dn] + zothers:
        pl.semaphore_signal(barrier, inc=1, device_id=(to,), device_id_type=MESH)
    mrow[...] = jnp.zeros_like(mrow)
    mrow[0:rows // 128, :] = mask_ref[...].astype(F32)
    xall[me, rows:rows + TAIL, :] = mrow[...].astype(BF16)
    w2p[...] = jnp.zeros_like(w2p)
    w2p[0:K, :] = w2_ref[...]
    w2b[...] = w2p[...].T.astype(BF16)
    w1b = w1_ref[...].astype(BF16)
    acc[...] = jnp.zeros_like(acc)
    x_copy.wait()
    pl.semaphore_wait(barrier, 7)

    is_mid = mid == 1

    def pick(i, values):
        out = values[0]
        for k in range(1, len(values)):
            out = jnp.where(i == k, values[k], out)
        return out

    def gather(buf, cuts, r_sem, s_sem, first, between_sends=None):
        def piece(b, c):
            return buf.at[b, pl.ds(cuts[c], cuts[c + 1] - cuts[c])]

        def wait_recv(b, c):
            rcopy(piece(b, c), piece(b, c), s_sem.at[0], r_sem.at[b, c], pn).wait_recv()

        def targets(c, q, j, between):
            to = []
            if q == 0 or c == 2:
                if j == 0:
                    to += [zin_n, zout_n] if between else [zin_n]
                elif between:
                    to += [zin_n if j == 1 else zout_n]
            if q == 0 and (c < 2 or j == 0):
                to += [xn, yn]
            elif (q == 2 and c < 2 and j % 2 == 0) or (q == 2 and c == 2 and j == 0):
                to += [xn]
            elif q == 1 and c < 2 and j % 2 == 1:
                to += [yn]
            return to + [pn]

        def multiply(ready, late):
            ids = [blocks[q, j, 0] for q, j in ready] + [blocks[q, j, 1] for q, j in late]
            if not ids:
                return

            def body(i, carry):
                b = pick(i, ids)
                if late:
                    @pl.when(i >= len(ready))
                    def _():
                        for c in range(PIECES):
                            wait_recv(b, c)
                if first:
                    a_copy(b).wait()
                acc[...] += jnp.dot(a_v[b], buf[b, 0:rows, :], preferred_element_type=F32)
                return carry
            lax.fori_loop(0, len(ids), body, 0)

        def run(order, between, pending):
            own_left = PIECES
            for step in program(order):
                if len(step) == 2:
                    multiply(*step)
                    continue
                own_left -= step[1:] == (0, 0)
                if step[1:] != (0, 0) and own_left == 0:
                    own_left = -1
                    if between_sends is not None:
                        between_sends()
                c, q, j = step
                b = blocks[q, j, 0]
                if (q, j) != (0, 0):
                    wait_recv(b, c)
                for to in targets(c, q, j, between):
                    k = len(pending)
                    rcopy(piece(b, c), piece(b, c), s_sem.at[k], r_sem.at[b, c], to).start()
                    pending.append((b, c, to))

        sent = {True: [], False: []}

        @pl.when(is_mid)
        def _():
            run(ORDER_MID, True, sent[True])

        @pl.when(mid == 0)
        def _():
            run(ORDER_END, False, sent[False])

        def drain():
            for between, when in ((True, is_mid), (False, mid == 0)):
                @pl.when(when)
                def _():
                    for k, (b, c, to) in enumerate(sent[between]):
                        rcopy(piece(b, c), piece(b, c), s_sem.at[k], r_sem.at[b, c], to).wait_send()
        return drain

    cuts1 = (0, rows * 3 // 8, rows * 6 // 8, rows + TAIL)
    cuts2 = (0, rows * 3 // 8, rows * 6 // 8, rows)
    drain1 = gather(xall, cuts1, ag1_r, ag1_s, True)

    s1b = acc[...].astype(BF16)
    s1[...] = s1b
    z1 = jnp.dot(s1b, w1b, preferred_element_type=F32)
    hall[me] = jnp.maximum(z1, 0.0).astype(BF16)
    sq[...] = z1
    acc[...] = jnp.zeros_like(acc)

    def count_body(b, tot):
        return tot + xall[b, rows:rows + TAIL, :].astype(F32)

    def early():
        z1t[...] = sq[...].T
        s1t[...] = s1[...].astype(F32).T.astype(BF16)
        cnt[...] = lax.fori_loop(0, NDEV, count_body, jnp.zeros((TAIL, 128), F32))

    drain2 = gather(hall, cuts2, ag2_r, ag2_s, False, early)

    w2t = w2p[0:KP, :].astype(BF16)
    label_count = jnp.sum(cnt[...])
    s2b = acc[...].astype(BF16)
    z2 = lax.dot_general(w2t, s2b, (((1,), (1,)), ((), ())), preferred_element_type=F32)
    row_id = lax.broadcasted_iota(jnp.int32, (KP, rows), 0)
    valid = row_id < K
    top = jnp.max(jnp.where(valid, z2, -jnp.inf), axis=0, keepdims=True)
    shifted = jnp.where(valid, z2 - top, 0.0)
    norm = jnp.log(jnp.sum(jnp.where(valid, jnp.exp(shifted), 0.0), axis=0, keepdims=True))
    log_prob = shifted - norm
    hot = row_id == lab_ref[...]
    onehot = jnp.where(hot, 1.0, 0.0)
    weight = jnp.concatenate([mrow[k:k + 1, :] for k in range(rows // 128)], axis=1)
    loss_row = -weight * jnp.sum(jnp.where(hot, log_prob, 0.0), axis=0, keepdims=True)
    g2 = jnp.where(valid, weight * (jnp.exp(log_prob) - onehot) / label_count, 0.0).astype(BF16)
    ut[...] = jnp.dot(w2b[:, 0:KP], g2, preferred_element_type=F32).astype(BF16)
    dw2t = jnp.dot(g2, s2b, preferred_element_type=F32)
    loss_part = loss_row[:, 0:128]
    for k in range(1, rows // 128):
        loss_part = loss_part + loss_row[:, k * 128:(k + 1) * 128]
    ar2_src[...] = dw2t
    ar2_src[K:K + 1, :] = loss_part

    plane = y * 2 + x

    def make_ar(src, pin, pl4, zz, fin, s_sem, r_sem):
        n = src.shape[0] // 2

        def give():
            lo = pl.multiple_of((1 - core) * n, n)
            return [rcopy(src.at[pl.ds(lo, n)], pin, s_sem.at[0], r_sem.at[0], pn)]

        def over_plane():
            return [rcopy(pl4.at[plane], pl4.at[plane], s_sem.at[1 + k], r_sem.at[1 + plane], to)
                    for k, to in enumerate((xn, yn, dn))]

        def over_line():
            return [rcopy(zz.at[z], zz.at[z], s_sem.at[4 + k], r_sem.at[5 + z], to) for k, to in enumerate(zothers)]

        def back():
            return [rcopy(fin.at[core], fin.at[core], s_sem.at[7], r_sem.at[9], pn)]

        def start(copies):
            for c in copies:
                c.start()

        def s1():
            start(give())

        def s2():
            rcopy(pin, pin, s_sem.at[0], r_sem.at[0], pn).wait_recv()
            lo = pl.multiple_of(core * n, n)
            pl4[plane] = src[pl.ds(lo, n), :] + pin[...]
            start(over_plane())

        def s3():
            for px, py in ((1, 0), (0, 1), (1, 1)):
                p = (y + py * (1 - 2 * y)) * 2 + x + px * (1 - 2 * x)
                rcopy(pl4.at[p], pl4.at[p], s_sem.at[0], r_sem.at[1 + p], pn).wait_recv()
            zz[z] = (pl4[0] + pl4[1]) + (pl4[2] + pl4[3])
            start(over_line())

        def s4():
            for k in (1, 2, 3):
                o = (z + k) % 4
                rcopy(zz.at[o], zz.at[o], s_sem.at[0], r_sem.at[5 + o], pn).wait_recv()
            fin[core] = (zz[0] + zz[1]) + (zz[2] + zz[3])
            start(back())

        def s5():
            rcopy(fin.at[1 - core], fin.at[1 - core], s_sem.at[0], r_sem.at[9], pn).wait_recv()
            for c in give() + over_plane() + over_line() + back():
                c.wait_send()

        return s1, s2, s3, s4, s5

    small = make_ar(ar2_src, ar2_pin, ar2_pl, ar2_zz, ar2_fin, ar2_s, ar2_r)
    small[0]()

    def parts(q, j):
        i = q * 4 + j
        outbox[i] = jnp.dot(ut[...], a_v[bid(q, j, 1)], preferred_element_type=F32)
        rcopy(outbox.at[i], pairin.at[i], rs_ps.at[i], rs_pr.at[i], pn).start()
        own[i] = jnp.dot(ut[...], a_v[bid(q, j)], preferred_element_type=F32)

    def diag_body(k, carry):
        parts(3, 3 - k)
        return carry

    def side_body(k, carry):
        parts(1 + k % 2, 3 - k // 2)
        return carry

    def own_body(k, carry):
        parts(0, 3 - k)
        return carry

    def piece_rows(c):
        return pl.ds(CUTS[c], CUTS[c + 1] - CUTS[c])

    def landed(ref, sem):
        rcopy(ref, ref, rs_s.at[0], sem, pn).wait_recv()

    to_line = zin_n + mid * (zout_n - zin_n)
    mid_slot = {3: 3, 2: 2, 1: 5, 0: 0}
    line_slot = {3: 3 + 2 * mid, 2: 2 + 2 * mid, 1: 4 * mid}
    line_to = {3: zin_n, 2: zin_n, 1: to_line}

    def reduce_copy(k, i, c, dst, slot, r_sem, r_slot, to):
        target = dst.at[slot] if dst is zinb else dst.at[slot, piece_rows(c)]
        return rcopy(own.at[i, piece_rows(c)], target, rs_s.at[k], r_sem.at[r_slot], to)

    def reduce(order, between, sent):
        added = set()

        def value(q, j):
            i = q * 4 + j
            if i not in added:
                added.add(i)
                rcopy(pairin.at[i], pairin.at[i], rs_ps.at[0], rs_pr.at[i], pn).wait_recv()
                own[i] = own[i] + pairin[i]
            return i

        def send(i, dst, slot, r_sem, r_slot, to):
            sent.append((i, c, dst, slot, r_sem, r_slot, to))
            reduce_copy(len(sent) - 1, *sent[-1]).start()

        for code in order:
            kind, c, q, j = code // 64, code // 16 % 4, code // 4 % 4, code % 4
            if kind == CALC:
                if j == 1:
                    lax.fori_loop(0, 4, diag_body, 0)
                elif j == 2:
                    lax.fori_loop(0, 8, side_body, 0)
                    small[1]()
                else:
                    lax.fori_loop(0, 4, own_body, 0)
                continue
            hs = piece_rows(c)
            diag = (3 - j) // 2
            if kind == DIAG:
                i = value(3, j)
                if j % 2 == 1:
                    send(i, xin, diag, rs_xr, (diag, c), xn)
                else:
                    send(i, yin, diag, rs_yr, (diag, c), yn)
            elif kind == XSIDE:
                i = value(1, j)
                if j % 2 == 0:
                    landed(yin.at[diag, hs], rs_yr.at[diag, c])
                    own[i, hs] = own[i, hs] + yin[diag, hs]
                send(i, xin, 2 + j, rs_xr, (2 + j, c), xn)
            elif kind == YSIDE:
                i = value(2, j)
                if j % 2 == 1:
                    landed(xin.at[diag, hs], rs_xr.at[diag, c])
                    own[i, hs] = own[i, hs] + xin[diag, hs]
                send(i, yin, 2 + j, rs_yr, (2 + j, c), yn)
            elif kind == LINE:
                i = value(0, j)
                landed(xin.at[2 + j, hs], rs_xr.at[2 + j, c])
                landed(yin.at[2 + j, hs], rs_yr.at[2 + j, c])
                own[i, hs] = (own[i, hs] + xin[2 + j, hs]) + yin[2 + j, hs]
                for t in ([mid_slot[j]] if between else []) + ([4] if j == 0 else []):
                    landed(zin.at[t, hs], rs_zr.at[t, c])
                    own[i, hs] = own[i, hs] + zin[t, hs]
                if j > 0:
                    send(i, zin, line_slot[j], rs_zr, (line_slot[j], c), line_to[j])
            elif kind == BACK:
                i = value(q, j)
                for t in ([mid_slot[j]] if between else []) + ([4] if j == 0 else []):
                    landed(zinb.at[q, t], rs_br.at[q, t])
                    own[i, hs] = own[i, hs] + zinb[q, t]
                if j > 0:
                    send(i, zinb, (q, line_slot[j]), rs_br, (q, line_slot[j]), line_to[j])
            elif kind == BDIAG:
                send(12, xin, 0, rs_xr, (0, c), xn)
            elif kind == BX:
                send(4, xin, 2, rs_xr, (2, c), xn)
            elif kind == BY:
                landed(xin.at[0, hs], rs_xr.at[0, c])
                own[8, hs] = own[8, hs] + xin[0, hs]
                send(8, yin, 2, rs_yr, (2, c), yn)
            else:
                landed(xin.at[2, hs], rs_xr.at[2, c])
                landed(yin.at[2, hs], rs_yr.at[2, c])
                own[0, hs] = (own[0, hs] + xin[2, hs]) + yin[2, hs]
            steps_left = len(order) - 1 - order.index(code)
            if steps_left == 24:
                small[2]()
            elif steps_left == 6:
                small[3]()

    reduced = {True: [], False: []}

    @pl.when(is_mid)
    def _():
        reduce(REDUCE_MID, True, reduced[True])

    @pl.when(mid == 0)
    def _():
        reduce(REDUCE_END, False, reduced[False])

    g1t = jnp.where(z1t[...] > 0.0, own[0], 0.0).astype(BF16)
    ar1_src[...] = lax.dot_general(s1t[...], g1t, (((1,), (1,)), ((), ())), preferred_element_type=F32)
    big = make_ar(ar1_src, ar1_pin, ar1_pl, ar1_zz, ar1_fin, ar1_s, ar1_r)
    big[0]()
    small[4]()
    out_ref[F:F + KP // 2, :] = ar2_fin[0]
    out_ref[F + KP // 2:F + KP, :] = ar2_fin[1]
    loss_row = out_ref[F + K:F + K + 1, :]
    out_ref[F + K:F + K + 1, :] = jnp.sum(loss_row, axis=1, keepdims=True) / label_count + jnp.zeros_like(loss_row)
    big[1]()
    drain1()
    drain2()
    big[2]()
    for between, when in ((True, is_mid), (False, mid == 0)):
        @pl.when(when)
        def _():
            for k, spec in enumerate(reduced[between]):
                reduce_copy(k, *spec).wait_send()
    for i in range(16):
        rcopy(outbox.at[i], pairin.at[i], rs_ps.at[i], rs_pr.at[i], pn).wait_send()
    big[3]()
    big[4]()
    out_ref[0:F // 2, :] = ar1_fin[0]
    out_ref[F // 2:F, :] = ar1_fin[1]


def unpack(packed, loss_out, dw1_out, dw2_out):
    loss_out[0] = packed[F + K, 0]
    dw1_out[...] = packed[0:F, :]
    dw2_out[...] = packed[F:F + K, :]


def solution(mesh):
    axis = 'nodes'

    def local_step(adj_rows, feat_rows, w_one, w_two, label_rows, mask_rows):
        rows = adj_rows.shape[0]
        dma = pltpu.SemaphoreType.DMA
        nsend = 144
        blk = lambda n: pltpu.VMEM((n, F, rows), F32)
        ar = lambda n: [pltpu.VMEM((2 * n, F), F32), pltpu.VMEM((n, F), F32), pltpu.VMEM((4, n, F), F32),
                        pltpu.VMEM((4, n, F), F32), pltpu.VMEM((2, n, F), F32)]
        vmem = pl.BlockSpec(memory_space=pltpu.VMEM)
        hbm = pl.BlockSpec(memory_space=pl.ANY)
        packed = pl.pallas_call(
            functools.partial(kernel, axis, rows),
            name='gcn_step',
            out_shape=jax.ShapeDtypeStruct((F + KP, F), F32),
            in_specs=[hbm, hbm, vmem, vmem, vmem, vmem],
            out_specs=vmem,
            scratch_shapes=[
                pltpu.VMEM((NDEV, rows, rows), BF16), pltpu.VMEM((NDEV, rows + TAIL, F), BF16),
                pltpu.VMEM((NDEV, rows, F), BF16), pltpu.VMEM((rows, F), F32), pltpu.VMEM((rows, F), BF16),
                pltpu.VMEM((F, rows), BF16), pltpu.VMEM((F, rows), F32), pltpu.VMEM((F, F), F32),
                pltpu.VMEM((F, F), BF16), pltpu.VMEM((F, rows), BF16), pltpu.VMEM((TAIL, F), F32), pltpu.VMEM((TAIL, F), F32),
                pltpu.VMEM((rows, F), F32),
                blk(16), blk(16), blk(16), blk(6), blk(6), blk(6),
                pltpu.VMEM((4, 6, F - CUTS[-2], rows), F32),
                *ar(F // 2), *ar(KP // 2),
                dma((NDEV,)), dma(()), dma((NDEV, PIECES)), dma((nsend,)), dma((NDEV, PIECES)), dma((nsend,)),
                dma((16,)), dma((16,)), dma((64,)), dma((6, 3)), dma((6, 3)), dma((6, 3)), dma((4, 6)), dma((8,)), dma((10,)), dma((8,)), dma((10,)),
            ],
            compiler_params=pltpu.CompilerParams(collective_id=0, has_side_effects=True,
                                                 vmem_limit_bytes=60 * 1024 * 1024),
        )(adj_rows, feat_rows, w_one, w_two.T, label_rows.reshape(1, rows), mask_rows.reshape(rows // 128, 128))
        loss, dw_one, dw_two_t = pl.pallas_call(
            unpack,
            name='unpack',
            out_shape=(jax.ShapeDtypeStruct((1,), F32), jax.ShapeDtypeStruct((F, F), F32),
                       jax.ShapeDtypeStruct((K, F), F32)),
            in_specs=[vmem],
            out_specs=(pl.BlockSpec(memory_space=pltpu.SMEM), vmem, vmem),
        )(packed)
        return loss, dw_one, dw_two_t.T

    return jax.shard_map(local_step, mesh=mesh,
                         in_specs=(P(axis, None), P(axis, None), P(None, None), P(None, None), P(axis), P(axis)),
                         out_specs=(P(None), P(None, None), P(None, None)), check_vma=False)
```

```python
import functools

import jax
import jax.numpy as jnp
from jax import lax
from jax.experimental import pallas as pl
from jax.experimental.pallas import tpu as pltpu
from jax.sharding import PartitionSpec as P

MESH = pl.DeviceIdType.MESH
F32 = jnp.float32
BF16 = jnp.bfloat16
NDEV = 32
F = 128
K = 40
KP = 48
TAIL = 16

ORDER_END = (
    0, 32, 16, 8, 36, 40, 17, 33, 1, 12, 2, 44, 4, 25, 21, 24, 5, 18, 9, 3, 6, 37, 19, 20,
    10, 28, 41, 22, 45, 26, 7, 43, 34, 23, 42, 39, 13, 29, 11, 35, 15, 38, 14, 27, 30, 46, 47, 31,
)
ORDER_MID = (
    0, 16, 32, 1, 2, 18, 36, 34, 40, 5, 17, 9, 3, 37, 41, 33, 42, 19, 45, 39, 8, 10, 24, 44,
    4, 20, 21, 7, 11, 43, 47, 27, 35, 38, 23, 46, 22, 25, 29, 26, 12, 6, 15, 13, 31, 14, 28, 30,
)
PIECES = 3
BATCH = 4

CALC, DIAG, XSIDE, YSIDE, LINE, BACK, BDIAG, BX, BY, BEND = range(10)
CUTS = (0, 56, 104, 128)
REDUCE_END = (
    1, 67, 367, 66, 366, 81, 365, 82, 2, 362, 83, 195, 363, 358, 131, 359, 64, 65, 146, 361, 3, 355, 194, 210,
    211, 354, 353, 147, 357, 193, 80, 209, 145, 130, 259, 364, 128, 274, 129, 275, 258, 416, 356, 144, 192, 273, 360, 352,
    208, 257, 544, 480, 272, 256, 608,
)
REDUCE_MID = (
    1, 67, 82, 81, 64, 83, 2, 66, 131, 366, 65, 367, 80, 195, 362, 363, 210, 147, 358, 361, 364, 365, 3, 359,
    355, 211, 130, 354, 353, 193, 194, 146, 356, 145, 129, 259, 416, 144, 357, 209, 360, 128, 274, 480, 208, 275, 257, 192,
    273, 258, 352, 544, 272, 256, 608,
)


def program(order):
    seen, steps, ready, late, following = {}, [], [], [], []
    for code in order:
        c, q, j = code // 16, code // 4 % 4, code % 4
        steps.append((c, q, j))
        seen[q, j] = seen.get((q, j), 0) + 1
        if seen[q, j] == PIECES:
            ready.append((q, j))
            following.append((q, j))
            if len(ready) + len(late) >= BATCH:
                steps.append((ready, late))
                ready, late, following = [], following, []
    return steps + [(ready, late), ([], following)]


def kernel(axis, rows, a_hbm, x_hbm, w1_ref, w2_ref, lab_ref, mask_ref, out_ref,
           a_v, xall, hall, acc, s1, s1t, z1t, w2p, w2b, ut, mrow, cnt, sq,
           own, outbox, pairin, xin, yin, zin, zinb,
           ar1_src, ar1_pin, ar1_pl, ar1_zz, ar1_fin, ar2_src, ar2_pin, ar2_pl, ar2_zz, ar2_fin,
           a_sem, x_sem, ag1_r, ag1_s, ag2_r, ag2_s, rs_ps, rs_pr, rs_s, rs_xr, rs_yr, rs_zr, rs_br,
           ar1_s, ar1_r, ar2_s, ar2_r):
    me = lax.axis_index(axis)
    core = me % 2
    x = (me // 2) % 2
    y = (me // 4) % 2
    z = me // 8
    mid = ((z + 1) // 2) % 2
    half = z // 2
    z_in = 1 + z % 2
    z_out = (3 * z - 3) * mid + z * (1 - mid)

    def dev(xx, yy, zz, cc):
        return ((zz * 2 + yy) * 2 + xx) * 2 + cc

    xn, yn = dev(1 - x, y, z, core), dev(x, 1 - y, z, core)
    dn, pn = dev(1 - x, 1 - y, z, core), dev(x, y, z, 1 - core)
    zin_n, zout_n = dev(x, y, z_in, core), dev(x, y, z_out, core)
    zothers = [dev(x, y, (z + k) % 4, core) for k in (1, 2, 3)]

    def zk(j):
        late = j // 2
        line = late * j + (1 - late) * (j + mid * (1 - 2 * j))
        return line + half * (3 - 2 * line)

    def bid(q, j, other=0):
        qx, qy = q % 2, q // 2
        cc = core + other * (1 - 2 * core)
        return dev(x + qx * (1 - 2 * x), y + qy * (1 - 2 * y), zk(j), cc)

    def rcopy(src, dst, ssem, rsem, to):
        return pltpu.make_async_remote_copy(src_ref=src, dst_ref=dst, send_sem=ssem, recv_sem=rsem, device_id=(to,),
                                            device_id_type=MESH)

    def a_copy(b):
        cols = pl.ds(pl.multiple_of(b * rows, rows), rows)
        return pltpu.make_async_copy(a_hbm.at[:, cols], a_v.at[b], a_sem.at[b])

    x_copy = pltpu.make_async_copy(x_hbm, xall.at[me, pl.ds(0, rows)], x_sem)
    x_copy.start()
    blocks = {(q, j, o): bid(q, j, o) for q in range(4) for j in range(4) for o in range(2)}
    for b in blocks.values():
        a_copy(b).start()
    barrier = pltpu.get_barrier_semaphore()
    for to in [pn, xn, yn, dn] + zothers:
        pl.semaphore_signal(barrier, inc=1, device_id=(to,), device_id_type=MESH)
    mrow[...] = jnp.zeros_like(mrow)
    mrow[0:rows // 128, :] = mask_ref[...].astype(F32)
    xall[me, rows:rows + TAIL, :] = mrow[...].astype(BF16)
    w2p[...] = jnp.zeros_like(w2p)
    w2p[0:K, :] = w2_ref[...]
    w2b[...] = w2p[...].T.astype(BF16)
    w1b = w1_ref[...].astype(BF16)
    acc[...] = jnp.zeros_like(acc)
    x_copy.wait()
    pl.semaphore_wait(barrier, 7)

    is_mid = mid == 1

    def pick(i, values):
        out = values[0]
        for k in range(1, len(values)):
            out = jnp.where(i == k, values[k], out)
        return out

    def gather(buf, cuts, r_sem, s_sem, first, between_sends=None):
        def piece(b, c):
            return buf.at[b, pl.ds(cuts[c], cuts[c + 1] - cuts[c])]

        def wait_recv(b, c):
            rcopy(piece(b, c), piece(b, c), s_sem.at[0], r_sem.at[b, c], pn).wait_recv()

        def targets(c, q, j, between):
            to = []
            if q == 0 or c == 2:
                if j == 0:
                    to += [zin_n, zout_n] if between else [zin_n]
                elif between:
                    to += [zin_n if j == 1 else zout_n]
            if q == 0 and (c < 2 or j == 0):
                to += [xn, yn]
            elif (q == 2 and c < 2 and j % 2 == 0) or (q == 2 and c == 2 and j == 0):
                to += [xn]
            elif q == 1 and c < 2 and j % 2 == 1:
                to += [yn]
            return to + [pn]

        def multiply(ready, late):
            ids = [blocks[q, j, 0] for q, j in ready] + [blocks[q, j, 1] for q, j in late]
            if not ids:
                return

            def body(i, carry):
                b = pick(i, ids)
                if late:
                    @pl.when(i >= len(ready))
                    def _():
                        for c in range(PIECES):
                            wait_recv(b, c)
                if first:
                    a_copy(b).wait()
                acc[...] += jnp.dot(a_v[b], buf[b, 0:rows, :], preferred_element_type=F32)
                return carry
            lax.fori_loop(0, len(ids), body, 0)

        def run(order, between, pending):
            own_left = PIECES
            for step in program(order):
                if len(step) == 2:
                    multiply(*step)
                    continue
                own_left -= step[1:] == (0, 0)
                if step[1:] != (0, 0) and own_left == 0:
                    own_left = -1
                    if between_sends is not None:
                        between_sends()
                c, q, j = step
                b = blocks[q, j, 0]
                if (q, j) != (0, 0):
                    wait_recv(b, c)
                for to in targets(c, q, j, between):
                    k = len(pending)
                    rcopy(piece(b, c), piece(b, c), s_sem.at[k], r_sem.at[b, c], to).start()
                    pending.append((b, c, to))

        sent = {True: [], False: []}

        @pl.when(is_mid)
        def _():
            run(ORDER_MID, True, sent[True])

        @pl.when(mid == 0)
        def _():
            run(ORDER_END, False, sent[False])

        def drain():
            for between, when in ((True, is_mid), (False, mid == 0)):
                @pl.when(when)
                def _():
                    for k, (b, c, to) in enumerate(sent[between]):
                        rcopy(piece(b, c), piece(b, c), s_sem.at[k], r_sem.at[b, c], to).wait_send()
        return drain

    cuts1 = (0, rows * 13 // 32, rows * 26 // 32, rows + TAIL)
    cuts2 = (0, rows * 13 // 32, rows * 26 // 32, rows)
    drain1 = gather(xall, cuts1, ag1_r, ag1_s, True)

    s1b = acc[...].astype(BF16)
    s1[...] = s1b
    z1 = jnp.dot(s1b, w1b, preferred_element_type=F32)
    hall[me] = jnp.maximum(z1, 0.0).astype(BF16)
    sq[...] = z1
    acc[...] = jnp.zeros_like(acc)

    def count_body(b, tot):
        return tot + xall[b, rows:rows + TAIL, :].astype(F32)

    def early():
        z1t[...] = sq[...].T
        s1t[...] = s1[...].astype(F32).T.astype(BF16)
        cnt[...] = lax.fori_loop(0, NDEV, count_body, jnp.zeros((TAIL, 128), F32))

    drain2 = gather(hall, cuts2, ag2_r, ag2_s, False, early)

    w2t = w2p[0:KP, :].astype(BF16)
    label_count = jnp.sum(cnt[...])
    s2b = acc[...].astype(BF16)
    z2 = lax.dot_general(w2t, s2b, (((1,), (1,)), ((), ())), preferred_element_type=F32)
    row_id = lax.broadcasted_iota(jnp.int32, (KP, rows), 0)
    valid = row_id < K
    top = jnp.max(jnp.where(valid, z2, -jnp.inf), axis=0, keepdims=True)
    shifted = jnp.where(valid, z2 - top, 0.0)
    norm = jnp.log(jnp.sum(jnp.where(valid, jnp.exp(shifted), 0.0), axis=0, keepdims=True))
    log_prob = shifted - norm
    hot = row_id == lab_ref[...]
    onehot = jnp.where(hot, 1.0, 0.0)
    weight = jnp.concatenate([mrow[k:k + 1, :] for k in range(rows // 128)], axis=1)
    loss_row = -weight * jnp.sum(jnp.where(hot, log_prob, 0.0), axis=0, keepdims=True)
    g2 = jnp.where(valid, weight * (jnp.exp(log_prob) - onehot) / label_count, 0.0).astype(BF16)
    ut[...] = jnp.dot(w2b[:, 0:KP], g2, preferred_element_type=F32).astype(BF16)
    dw2t = jnp.dot(g2, s2b, preferred_element_type=F32)
    loss_part = loss_row[:, 0:128]
    for k in range(1, rows // 128):
        loss_part = loss_part + loss_row[:, k * 128:(k + 1) * 128]
    ar2_src[...] = dw2t
    ar2_src[K:K + 1, :] = loss_part

    plane = y * 2 + x

    def make_ar(src, pin, pl4, zz, fin, s_sem, r_sem):
        n = src.shape[0] // 2

        def give():
            lo = pl.multiple_of((1 - core) * n, n)
            return [rcopy(src.at[pl.ds(lo, n)], pin, s_sem.at[0], r_sem.at[0], pn)]

        def over_plane():
            return [rcopy(pl4.at[plane], pl4.at[plane], s_sem.at[1 + k], r_sem.at[1 + plane], to)
                    for k, to in enumerate((xn, yn, dn))]

        def over_line():
            return [rcopy(zz.at[z], zz.at[z], s_sem.at[4 + k], r_sem.at[5 + z], to) for k, to in enumerate(zothers)]

        def back():
            return [rcopy(fin.at[core], fin.at[core], s_sem.at[7], r_sem.at[9], pn)]

        def start(copies):
            for c in copies:
                c.start()

        def s1():
            start(give())

        def s2():
            rcopy(pin, pin, s_sem.at[0], r_sem.at[0], pn).wait_recv()
            lo = pl.multiple_of(core * n, n)
            pl4[plane] = src[pl.ds(lo, n), :] + pin[...]
            start(over_plane())

        def s3():
            for px, py in ((1, 0), (0, 1), (1, 1)):
                p = (y + py * (1 - 2 * y)) * 2 + x + px * (1 - 2 * x)
                rcopy(pl4.at[p], pl4.at[p], s_sem.at[0], r_sem.at[1 + p], pn).wait_recv()
            zz[z] = (pl4[0] + pl4[1]) + (pl4[2] + pl4[3])
            start(over_line())

        def s4():
            for k in (1, 2, 3):
                o = (z + k) % 4
                rcopy(zz.at[o], zz.at[o], s_sem.at[0], r_sem.at[5 + o], pn).wait_recv()
            fin[core] = (zz[0] + zz[1]) + (zz[2] + zz[3])
            start(back())

        def s5():
            rcopy(fin.at[1 - core], fin.at[1 - core], s_sem.at[0], r_sem.at[9], pn).wait_recv()
            for c in give() + over_plane() + over_line() + back():
                c.wait_send()

        return s1, s2, s3, s4, s5

    small = make_ar(ar2_src, ar2_pin, ar2_pl, ar2_zz, ar2_fin, ar2_s, ar2_r)
    small[0]()

    def parts(q, j):
        i = q * 4 + j
        outbox[i] = jnp.dot(ut[...], a_v[bid(q, j, 1)], preferred_element_type=F32)
        rcopy(outbox.at[i], pairin.at[i], rs_ps.at[i], rs_pr.at[i], pn).start()
        own[i] = jnp.dot(ut[...], a_v[bid(q, j)], preferred_element_type=F32)

    def diag_body(k, carry):
        parts(3, 3 - k)
        return carry

    def side_body(k, carry):
        parts(1 + k % 2, 3 - k // 2)
        return carry

    def own_body(k, carry):
        parts(0, 3 - k)
        return carry

    def piece_rows(c):
        return pl.ds(CUTS[c], CUTS[c + 1] - CUTS[c])

    def landed(ref, sem):
        rcopy(ref, ref, rs_s.at[0], sem, pn).wait_recv()

    to_line = zin_n + mid * (zout_n - zin_n)
    mid_slot = {3: 3, 2: 2, 1: 5, 0: 0}
    line_slot = {3: 3 + 2 * mid, 2: 2 + 2 * mid, 1: 4 * mid}
    line_to = {3: zin_n, 2: zin_n, 1: to_line}

    def reduce_copy(k, i, c, dst, slot, r_sem, r_slot, to):
        target = dst.at[slot] if dst is zinb else dst.at[slot, piece_rows(c)]
        return rcopy(own.at[i, piece_rows(c)], target, rs_s.at[k], r_sem.at[r_slot], to)

    def reduce(order, between, sent):
        added = set()

        def value(q, j):
            i = q * 4 + j
            if i not in added:
                added.add(i)
                rcopy(pairin.at[i], pairin.at[i], rs_ps.at[0], rs_pr.at[i], pn).wait_recv()
                own[i] = own[i] + pairin[i]
            return i

        def send(i, dst, slot, r_sem, r_slot, to):
            sent.append((i, c, dst, slot, r_sem, r_slot, to))
            reduce_copy(len(sent) - 1, *sent[-1]).start()

        for code in order:
            kind, c, q, j = code // 64, code // 16 % 4, code // 4 % 4, code % 4
            if kind == CALC:
                if j == 1:
                    lax.fori_loop(0, 4, diag_body, 0)
                elif j == 2:
                    lax.fori_loop(0, 8, side_body, 0)
                    small[1]()
                else:
                    lax.fori_loop(0, 4, own_body, 0)
                continue
            hs = piece_rows(c)
            diag = (3 - j) // 2
            if kind == DIAG:
                i = value(3, j)
                if j % 2 == 1:
                    send(i, xin, diag, rs_xr, (diag, c), xn)
                else:
                    send(i, yin, diag, rs_yr, (diag, c), yn)
            elif kind == XSIDE:
                i = value(1, j)
                if j % 2 == 0:
                    landed(yin.at[diag, hs], rs_yr.at[diag, c])
                    own[i, hs] = own[i, hs] + yin[diag, hs]
                send(i, xin, 2 + j, rs_xr, (2 + j, c), xn)
            elif kind == YSIDE:
                i = value(2, j)
                if j % 2 == 1:
                    landed(xin.at[diag, hs], rs_xr.at[diag, c])
                    own[i, hs] = own[i, hs] + xin[diag, hs]
                send(i, yin, 2 + j, rs_yr, (2 + j, c), yn)
            elif kind == LINE:
                i = value(0, j)
                landed(xin.at[2 + j, hs], rs_xr.at[2 + j, c])
                landed(yin.at[2 + j, hs], rs_yr.at[2 + j, c])
                own[i, hs] = (own[i, hs] + xin[2 + j, hs]) + yin[2 + j, hs]
                for t in ([mid_slot[j]] if between else []) + ([4] if j == 0 else []):
                    landed(zin.at[t, hs], rs_zr.at[t, c])
                    own[i, hs] = own[i, hs] + zin[t, hs]
                if j > 0:
                    send(i, zin, line_slot[j], rs_zr, (line_slot[j], c), line_to[j])
            elif kind == BACK:
                i = value(q, j)
                for t in ([mid_slot[j]] if between else []) + ([4] if j == 0 else []):
                    landed(zinb.at[q, t], rs_br.at[q, t])
                    own[i, hs] = own[i, hs] + zinb[q, t]
                if j > 0:
                    send(i, zinb, (q, line_slot[j]), rs_br, (q, line_slot[j]), line_to[j])
            elif kind == BDIAG:
                send(12, xin, 0, rs_xr, (0, c), xn)
            elif kind == BX:
                send(4, xin, 2, rs_xr, (2, c), xn)
            elif kind == BY:
                landed(xin.at[0, hs], rs_xr.at[0, c])
                own[8, hs] = own[8, hs] + xin[0, hs]
                send(8, yin, 2, rs_yr, (2, c), yn)
            else:
                landed(xin.at[2, hs], rs_xr.at[2, c])
                landed(yin.at[2, hs], rs_yr.at[2, c])
                own[0, hs] = (own[0, hs] + xin[2, hs]) + yin[2, hs]
            steps_left = len(order) - 1 - order.index(code)
            if steps_left == 24:
                small[2]()
            elif steps_left == 6:
                small[3]()

    reduced = {True: [], False: []}

    @pl.when(is_mid)
    def _():
        reduce(REDUCE_MID, True, reduced[True])

    @pl.when(mid == 0)
    def _():
        reduce(REDUCE_END, False, reduced[False])

    g1t = jnp.where(z1t[...] > 0.0, own[0], 0.0).astype(BF16)
    ar1_src[...] = lax.dot_general(s1t[...], g1t, (((1,), (1,)), ((), ())), preferred_element_type=F32)
    big = make_ar(ar1_src, ar1_pin, ar1_pl, ar1_zz, ar1_fin, ar1_s, ar1_r)
    big[0]()
    small[4]()
    out_ref[F:F + KP // 2, :] = ar2_fin[0]
    out_ref[F + KP // 2:F + KP, :] = ar2_fin[1]
    loss_row = out_ref[F + K:F + K + 1, :]
    out_ref[F + K:F + K + 1, :] = jnp.sum(loss_row, axis=1, keepdims=True) / label_count + jnp.zeros_like(loss_row)
    big[1]()
    drain1()
    drain2()
    big[2]()
    for between, when in ((True, is_mid), (False, mid == 0)):
        @pl.when(when)
        def _():
            for k, spec in enumerate(reduced[between]):
                reduce_copy(k, *spec).wait_send()
    for i in range(16):
        rcopy(outbox.at[i], pairin.at[i], rs_ps.at[i], rs_pr.at[i], pn).wait_send()
    big[3]()
    big[4]()
    out_ref[0:F // 2, :] = ar1_fin[0]
    out_ref[F // 2:F, :] = ar1_fin[1]


def unpack(packed, loss_out, dw1_out, dw2_out):
    loss_out[0] = packed[F + K, 0]
    dw1_out[...] = packed[0:F, :]
    dw2_out[...] = packed[F:F + K, :]


def solution(mesh):
    axis = 'nodes'

    def local_step(adj_rows, feat_rows, w_one, w_two, label_rows, mask_rows):
        rows = adj_rows.shape[0]
        dma = pltpu.SemaphoreType.DMA
        nsend = 144
        blk = lambda n: pltpu.VMEM((n, F, rows), F32)
        ar = lambda n: [pltpu.VMEM((2 * n, F), F32), pltpu.VMEM((n, F), F32), pltpu.VMEM((4, n, F), F32),
                        pltpu.VMEM((4, n, F), F32), pltpu.VMEM((2, n, F), F32)]
        vmem = pl.BlockSpec(memory_space=pltpu.VMEM)
        hbm = pl.BlockSpec(memory_space=pl.ANY)
        packed = pl.pallas_call(
            functools.partial(kernel, axis, rows),
            name='gcn_step',
            out_shape=pltpu.VMEM((F + KP, F), F32),
            in_specs=[hbm, hbm, vmem, vmem, vmem, vmem],
            out_specs=vmem,
            scratch_shapes=[
                pltpu.VMEM((NDEV, rows, rows), BF16), pltpu.VMEM((NDEV, rows + TAIL, F), BF16),
                pltpu.VMEM((NDEV, rows, F), BF16), pltpu.VMEM((rows, F), F32), pltpu.VMEM((rows, F), BF16),
                pltpu.VMEM((F, rows), BF16), pltpu.VMEM((F, rows), F32), pltpu.VMEM((F, F), F32),
                pltpu.VMEM((F, F), BF16), pltpu.VMEM((F, rows), BF16), pltpu.VMEM((TAIL, F), F32), pltpu.VMEM((TAIL, F), F32),
                pltpu.VMEM((rows, F), F32),
                blk(16), blk(16), blk(16), blk(6), blk(6), blk(6),
                pltpu.VMEM((4, 6, F - CUTS[-2], rows), F32),
                *ar(F // 2), *ar(KP // 2),
                dma((NDEV,)), dma(()), dma((NDEV, PIECES)), dma((nsend,)), dma((NDEV, PIECES)), dma((nsend,)),
                dma((16,)), dma((16,)), dma((64,)), dma((6, 3)), dma((6, 3)), dma((6, 3)), dma((4, 6)), dma((8,)), dma((10,)), dma((8,)), dma((10,)),
            ],
            compiler_params=pltpu.CompilerParams(collective_id=0, has_side_effects=True,
                                                 vmem_limit_bytes=60 * 1024 * 1024),
        )(adj_rows, feat_rows, w_one, w_two.T, label_rows.reshape(1, rows), mask_rows.reshape(rows // 128, 128))
        loss, dw_one, dw_two_t = pl.pallas_call(
            unpack,
            name='unpack',
            out_shape=(jax.ShapeDtypeStruct((1,), F32), jax.ShapeDtypeStruct((F, F), F32),
                       jax.ShapeDtypeStruct((K, F), F32)),
            in_specs=[vmem],
            out_specs=(pl.BlockSpec(memory_space=pltpu.SMEM), vmem, vmem),
        )(pltpu.with_memory_space_constraint(packed, pltpu.VMEM))
        return loss, dw_one, dw_two_t.T

    return jax.shard_map(local_step, mesh=mesh,
                         in_specs=(P(axis, None), P(axis, None), P(None, None), P(None, None), P(axis), P(axis)),
                         out_specs=(P(None), P(None, None), P(None, None)), check_vma=False)
```

```python
import functools

import jax
import jax.numpy as jnp
from jax import lax
from jax.experimental import pallas as pl
from jax.experimental.pallas import tpu as pltpu
from jax.sharding import PartitionSpec as P

MESH = pl.DeviceIdType.MESH
F32 = jnp.float32
BF16 = jnp.bfloat16
NDEV = 32
F = 128
K = 40
KP = 48
TAIL = 16

ORDER_END = (
    0, 16, 32, 1, 17, 40, 8, 2, 36, 5, 18, 21, 33, 44, 37, 24, 3, 12, 19, 34, 38, 10, 22, 28,
    29, 13, 26, 4, 7, 9, 6, 45, 23, 43, 41, 42, 11, 20, 39, 27, 25, 15, 30, 14, 46, 35, 47, 31,
)
ORDER_MID = (
    0, 16, 32, 2, 1, 18, 17, 36, 40, 3, 19, 10, 41, 26, 24, 34, 5, 38, 37, 42, 21, 44, 33, 4,
    43, 11, 20, 7, 45, 39, 8, 23, 9, 46, 27, 35, 22, 47, 14, 25, 30, 6, 15, 31, 13, 28, 29, 12,
)
PIECES = 3
BATCH = 4

CALC, DIAG, XSIDE, YSIDE, LINE, BACK, BDIAG, BX, BY, BEND = range(10)
CUTS = (0, 56, 104, 128)
REDUCE_END = (
    1, 83, 82, 367, 66, 366, 67, 2, 362, 210, 81, 363, 358, 131, 146, 211, 3, 147, 359, 195, 357, 354, 365, 65,
    194, 355, 130, 145, 364, 64, 361, 353, 259, 275, 209, 80, 416, 129, 193, 208, 274, 258, 128, 273, 352, 356, 144, 480,
    360, 192, 257, 544, 256, 272, 608,
)
REDUCE_MID = (
    1, 83, 67, 82, 64, 2, 147, 367, 65, 66, 366, 80, 362, 365, 211, 195, 363, 146, 81, 358, 359, 3, 354, 210,
    361, 131, 357, 364, 355, 416, 193, 360, 145, 353, 194, 129, 209, 259, 544, 356, 208, 130, 128, 275, 274, 352, 144, 192,
    480, 257, 273, 258, 272, 256, 608,
)


def program(order):
    seen, steps, ready, late, following = {}, [], [], [], []
    for code in order:
        c, q, j = code // 16, code // 4 % 4, code % 4
        steps.append((c, q, j))
        seen[q, j] = seen.get((q, j), 0) + 1
        if seen[q, j] == PIECES:
            ready.append((q, j))
            following.append((q, j))
            if len(ready) + len(late) >= BATCH:
                steps.append((ready, late))
                ready, late, following = [], following, []
    return steps + [(ready, late), ([], following)]


def kernel(axis, rows, a_hbm, x_hbm, w1_ref, w2_ref, lab_ref, mask_ref, out_ref,
           a_v, xall, hall, acc, s1, s1t, z1t, w2p, w2b, ut, mrow, cnt, sq,
           own, outbox, pairin, xin, yin, zin, zinb,
           ar1_src, ar1_pin, ar1_pl, ar1_zz, ar1_fin, ar2_src, ar2_pin, ar2_pl, ar2_zz, ar2_fin,
           a_sem, x_sem, ag1_r, ag1_s, ag2_r, ag2_s, rs_ps, rs_pr, rs_s, rs_xr, rs_yr, rs_zr, rs_br,
           ar1_s, ar1_r, ar2_s, ar2_r):
    me = lax.axis_index(axis)
    core = me % 2
    x = (me // 2) % 2
    y = (me // 4) % 2
    z = me // 8
    mid = ((z + 1) // 2) % 2
    half = z // 2
    z_in = 1 + z % 2
    z_out = (3 * z - 3) * mid + z * (1 - mid)

    def dev(xx, yy, zz, cc):
        return ((zz * 2 + yy) * 2 + xx) * 2 + cc

    xn, yn = dev(1 - x, y, z, core), dev(x, 1 - y, z, core)
    dn, pn = dev(1 - x, 1 - y, z, core), dev(x, y, z, 1 - core)
    zin_n, zout_n = dev(x, y, z_in, core), dev(x, y, z_out, core)
    zothers = [dev(x, y, (z + k) % 4, core) for k in (1, 2, 3)]

    def zk(j):
        late = j // 2
        line = late * j + (1 - late) * (j + mid * (1 - 2 * j))
        return line + half * (3 - 2 * line)

    def bid(q, j, other=0):
        qx, qy = q % 2, q // 2
        cc = core + other * (1 - 2 * core)
        return dev(x + qx * (1 - 2 * x), y + qy * (1 - 2 * y), zk(j), cc)

    def rcopy(src, dst, ssem, rsem, to):
        return pltpu.make_async_remote_copy(src_ref=src, dst_ref=dst, send_sem=ssem, recv_sem=rsem, device_id=(to,),
                                            device_id_type=MESH)

    def a_copy(b):
        cols = pl.ds(pl.multiple_of(b * rows, rows), rows)
        return pltpu.make_async_copy(a_hbm.at[:, cols], a_v.at[b], a_sem.at[b])

    x_copy = pltpu.make_async_copy(x_hbm, xall.at[me, pl.ds(0, rows)], x_sem)
    x_copy.start()
    blocks = {(q, j, o): bid(q, j, o) for q in range(4) for j in range(4) for o in range(2)}
    for b in blocks.values():
        a_copy(b).start()
    barrier = pltpu.get_barrier_semaphore()
    for to in [pn, xn, yn, dn] + zothers:
        pl.semaphore_signal(barrier, inc=1, device_id=(to,), device_id_type=MESH)
    mrow[...] = jnp.zeros_like(mrow)
    mrow[0:rows // 128, :] = mask_ref[...].astype(F32)
    xall[me, rows:rows + TAIL, :] = mrow[...].astype(BF16)
    w2p[...] = jnp.zeros_like(w2p)
    w2p[0:K, :] = w2_ref[...]
    w2b[...] = w2p[...].T.astype(BF16)
    w1b = w1_ref[...].astype(BF16)
    acc[...] = jnp.zeros_like(acc)
    x_copy.wait()
    pl.semaphore_wait(barrier, 7)

    is_mid = mid == 1

    def pick(i, values):
        out = values[0]
        for k in range(1, len(values)):
            out = jnp.where(i == k, values[k], out)
        return out

    def gather(buf, cuts, r_sem, s_sem, first, between_sends=None):
        def piece(b, c):
            return buf.at[b, pl.ds(cuts[c], cuts[c + 1] - cuts[c])]

        def wait_recv(b, c):
            rcopy(piece(b, c), piece(b, c), s_sem.at[0], r_sem.at[b, c], pn).wait_recv()

        def targets(c, q, j, between):
            to = []
            if q == 0 or c == 2:
                if j == 0:
                    to += [zin_n, zout_n] if between else [zin_n]
                elif between:
                    to += [zin_n if j == 1 else zout_n]
            if q == 0 and (c < 2 or j == 0):
                to += [xn, yn]
            elif (q == 2 and c < 2 and j % 2 == 0) or (q == 2 and c == 2 and j == 0):
                to += [xn]
            elif q == 1 and c < 2 and j % 2 == 1:
                to += [yn]
            return to + [pn]

        def multiply(ready, late):
            ids = [blocks[q, j, 0] for q, j in ready] + [blocks[q, j, 1] for q, j in late]
            if not ids:
                return

            def body(i, carry):
                b = pick(i, ids)
                if late:
                    @pl.when(i >= len(ready))
                    def _():
                        for c in range(PIECES):
                            wait_recv(b, c)
                if first:
                    a_copy(b).wait()
                acc[...] += jnp.dot(a_v[b], buf[b, 0:rows, :], preferred_element_type=F32)
                return carry
            lax.fori_loop(0, len(ids), body, 0)

        def run(order, between, pending):
            own_left = PIECES
            for step in program(order):
                if len(step) == 2:
                    multiply(*step)
                    continue
                own_left -= step[1:] == (0, 0)
                if step[1:] != (0, 0) and own_left == 0:
                    own_left = -1
                    if between_sends is not None:
                        between_sends()
                c, q, j = step
                b = blocks[q, j, 0]
                if (q, j) != (0, 0):
                    wait_recv(b, c)
                for to in targets(c, q, j, between):
                    k = len(pending)
                    rcopy(piece(b, c), piece(b, c), s_sem.at[k], r_sem.at[b, c], to).start()
                    pending.append((b, c, to))

        sent = {True: [], False: []}

        @pl.when(is_mid)
        def _():
            run(ORDER_MID, True, sent[True])

        @pl.when(mid == 0)
        def _():
            run(ORDER_END, False, sent[False])

        def drain():
            for between, when in ((True, is_mid), (False, mid == 0)):
                @pl.when(when)
                def _():
                    for k, (b, c, to) in enumerate(sent[between]):
                        rcopy(piece(b, c), piece(b, c), s_sem.at[k], r_sem.at[b, c], to).wait_send()
        return drain

    cuts1 = (0, rows * 3 // 8, rows * 6 // 8, rows + TAIL)
    cuts2 = (0, rows * 3 // 8, rows * 6 // 8, rows)
    drain1 = gather(xall, cuts1, ag1_r, ag1_s, True)

    s1b = acc[...].astype(BF16)
    s1[...] = s1b
    z1 = jnp.dot(s1b, w1b, preferred_element_type=F32)
    hall[me] = jnp.maximum(z1, 0.0).astype(BF16)
    sq[...] = z1
    acc[...] = jnp.zeros_like(acc)

    def count_body(b, tot):
        return tot + xall[b, rows:rows + TAIL, :].astype(F32)

    def early():
        z1t[...] = sq[...].T
        s1t[...] = s1[...].astype(F32).T.astype(BF16)
        cnt[...] = lax.fori_loop(0, NDEV, count_body, jnp.zeros((TAIL, 128), F32))

    drain2 = gather(hall, cuts2, ag2_r, ag2_s, False, early)

    w2t = w2p[0:KP, :].astype(BF16)
    label_count = jnp.sum(cnt[...])
    s2b = acc[...].astype(BF16)
    z2 = lax.dot_general(w2t, s2b, (((1,), (1,)), ((), ())), preferred_element_type=F32)
    row_id = lax.broadcasted_iota(jnp.int32, (KP, rows), 0)
    valid = row_id < K
    top = jnp.max(jnp.where(valid, z2, -jnp.inf), axis=0, keepdims=True)
    shifted = jnp.where(valid, z2 - top, 0.0)
    norm = jnp.log(jnp.sum(jnp.where(valid, jnp.exp(shifted), 0.0), axis=0, keepdims=True))
    log_prob = shifted - norm
    hot = row_id == lab_ref[...]
    onehot = jnp.where(hot, 1.0, 0.0)
    weight = jnp.concatenate([mrow[k:k + 1, :] for k in range(rows // 128)], axis=1)
    loss_row = -weight * jnp.sum(jnp.where(hot, log_prob, 0.0), axis=0, keepdims=True)
    g2 = jnp.where(valid, weight * (jnp.exp(log_prob) - onehot) / label_count, 0.0).astype(BF16)
    ut[...] = jnp.dot(w2b[:, 0:KP], g2, preferred_element_type=F32).astype(BF16)
    dw2t = jnp.dot(g2, s2b, preferred_element_type=F32)
    loss_part = loss_row[:, 0:128]
    for k in range(1, rows // 128):
        loss_part = loss_part + loss_row[:, k * 128:(k + 1) * 128]
    ar2_src[...] = dw2t
    ar2_src[K:K + 1, :] = loss_part

    plane = y * 2 + x

    def make_ar(src, pin, pl4, zz, fin, s_sem, r_sem):
        n = src.shape[0] // 2

        def give():
            lo = pl.multiple_of((1 - core) * n, n)
            return [rcopy(src.at[pl.ds(lo, n)], pin, s_sem.at[0], r_sem.at[0], pn)]

        def over_plane():
            return [rcopy(pl4.at[plane], pl4.at[plane], s_sem.at[1 + k], r_sem.at[1 + plane], to)
                    for k, to in enumerate((xn, yn, dn))]

        def over_line():
            return [rcopy(zz.at[z], zz.at[z], s_sem.at[4 + k], r_sem.at[5 + z], to) for k, to in enumerate(zothers)]

        def back():
            return [rcopy(fin.at[core], fin.at[core], s_sem.at[7], r_sem.at[9], pn)]

        def start(copies):
            for c in copies:
                c.start()

        def s1():
            start(give())

        def s2():
            rcopy(pin, pin, s_sem.at[0], r_sem.at[0], pn).wait_recv()
            lo = pl.multiple_of(core * n, n)
            pl4[plane] = src[pl.ds(lo, n), :] + pin[...]
            start(over_plane())

        def s3():
            for px, py in ((1, 0), (0, 1), (1, 1)):
                p = (y + py * (1 - 2 * y)) * 2 + x + px * (1 - 2 * x)
                rcopy(pl4.at[p], pl4.at[p], s_sem.at[0], r_sem.at[1 + p], pn).wait_recv()
            zz[z] = (pl4[0] + pl4[1]) + (pl4[2] + pl4[3])
            start(over_line())

        def s4():
            for k in (1, 2, 3):
                o = (z + k) % 4
                rcopy(zz.at[o], zz.at[o], s_sem.at[0], r_sem.at[5 + o], pn).wait_recv()
            fin[core] = (zz[0] + zz[1]) + (zz[2] + zz[3])
            start(back())

        def s5():
            rcopy(fin.at[1 - core], fin.at[1 - core], s_sem.at[0], r_sem.at[9], pn).wait_recv()
            for c in give() + over_plane() + over_line() + back():
                c.wait_send()

        return s1, s2, s3, s4, s5

    small = make_ar(ar2_src, ar2_pin, ar2_pl, ar2_zz, ar2_fin, ar2_s, ar2_r)
    small[0]()

    def parts(q, j):
        i = q * 4 + j
        outbox[i] = jnp.dot(ut[...], a_v[bid(q, j, 1)], preferred_element_type=F32)
        rcopy(outbox.at[i], pairin.at[i], rs_ps.at[i], rs_pr.at[i], pn).start()
        own[i] = jnp.dot(ut[...], a_v[bid(q, j)], preferred_element_type=F32)

    def diag_body(k, carry):
        parts(3, 3 - k)
        return carry

    def side_body(k, carry):
        parts(1 + k % 2, 3 - k // 2)
        return carry

    def own_body(k, carry):
        parts(0, 3 - k)
        return carry

    def piece_rows(c):
        return pl.ds(CUTS[c], CUTS[c + 1] - CUTS[c])

    def landed(ref, sem):
        rcopy(ref, ref, rs_s.at[0], sem, pn).wait_recv()

    to_line = zin_n + mid * (zout_n - zin_n)
    mid_slot = {3: 3, 2: 2, 1: 5, 0: 0}
    line_slot = {3: 3 + 2 * mid, 2: 2 + 2 * mid, 1: 4 * mid}
    line_to = {3: zin_n, 2: zin_n, 1: to_line}

    def reduce_copy(k, i, c, dst, slot, r_sem, r_slot, to):
        target = dst.at[slot] if dst is zinb else dst.at[slot, piece_rows(c)]
        return rcopy(own.at[i, piece_rows(c)], target, rs_s.at[k], r_sem.at[r_slot], to)

    def reduce(order, between, sent):
        added = set()

        def value(q, j):
            i = q * 4 + j
            if i not in added:
                added.add(i)
                rcopy(pairin.at[i], pairin.at[i], rs_ps.at[0], rs_pr.at[i], pn).wait_recv()
                own[i] = own[i] + pairin[i]
            return i

        def send(i, dst, slot, r_sem, r_slot, to):
            sent.append((i, c, dst, slot, r_sem, r_slot, to))
            reduce_copy(len(sent) - 1, *sent[-1]).start()

        for code in order:
            kind, c, q, j = code // 64, code // 16 % 4, code // 4 % 4, code % 4
            if kind == CALC:
                if j == 1:
                    lax.fori_loop(0, 4, diag_body, 0)
                elif j == 2:
                    lax.fori_loop(0, 8, side_body, 0)
                    small[1]()
                else:
                    lax.fori_loop(0, 4, own_body, 0)
                continue
            hs = piece_rows(c)
            diag = (3 - j) // 2
            if kind == DIAG:
                i = value(3, j)
                if j % 2 == 1:
                    send(i, xin, diag, rs_xr, (diag, c), xn)
                else:
                    send(i, yin, diag, rs_yr, (diag, c), yn)
            elif kind == XSIDE:
                i = value(1, j)
                if j % 2 == 0:
                    landed(yin.at[diag, hs], rs_yr.at[diag, c])
                    own[i, hs] = own[i, hs] + yin[diag, hs]
                send(i, xin, 2 + j, rs_xr, (2 + j, c), xn)
            elif kind == YSIDE:
                i = value(2, j)
                if j % 2 == 1:
                    landed(xin.at[diag, hs], rs_xr.at[diag, c])
                    own[i, hs] = own[i, hs] + xin[diag, hs]
                send(i, yin, 2 + j, rs_yr, (2 + j, c), yn)
            elif kind == LINE:
                i = value(0, j)
                landed(xin.at[2 + j, hs], rs_xr.at[2 + j, c])
                landed(yin.at[2 + j, hs], rs_yr.at[2 + j, c])
                own[i, hs] = (own[i, hs] + xin[2 + j, hs]) + yin[2 + j, hs]
                for t in ([mid_slot[j]] if between else []) + ([4] if j == 0 else []):
                    landed(zin.at[t, hs], rs_zr.at[t, c])
                    own[i, hs] = own[i, hs] + zin[t, hs]
                if j > 0:
                    send(i, zin, line_slot[j], rs_zr, (line_slot[j], c), line_to[j])
            elif kind == BACK:
                i = value(q, j)
                for t in ([mid_slot[j]] if between else []) + ([4] if j == 0 else []):
                    landed(zinb.at[q, t], rs_br.at[q, t])
                    own[i, hs] = own[i, hs] + zinb[q, t]
                if j > 0:
                    send(i, zinb, (q, line_slot[j]), rs_br, (q, line_slot[j]), line_to[j])
            elif kind == BDIAG:
                send(12, xin, 0, rs_xr, (0, c), xn)
            elif kind == BX:
                send(4, xin, 2, rs_xr, (2, c), xn)
            elif kind == BY:
                landed(xin.at[0, hs], rs_xr.at[0, c])
                own[8, hs] = own[8, hs] + xin[0, hs]
                send(8, yin, 2, rs_yr, (2, c), yn)
            else:
                landed(xin.at[2, hs], rs_xr.at[2, c])
                landed(yin.at[2, hs], rs_yr.at[2, c])
                own[0, hs] = (own[0, hs] + xin[2, hs]) + yin[2, hs]
            steps_left = len(order) - 1 - order.index(code)
            if steps_left == 24:
                small[2]()
            elif steps_left == 6:
                small[3]()

    reduced = {True: [], False: []}

    @pl.when(is_mid)
    def _():
        reduce(REDUCE_MID, True, reduced[True])

    @pl.when(mid == 0)
    def _():
        reduce(REDUCE_END, False, reduced[False])

    g1t = jnp.where(z1t[...] > 0.0, own[0], 0.0).astype(BF16)
    ar1_src[...] = lax.dot_general(s1t[...], g1t, (((1,), (1,)), ((), ())), preferred_element_type=F32)
    big = make_ar(ar1_src, ar1_pin, ar1_pl, ar1_zz, ar1_fin, ar1_s, ar1_r)
    big[0]()
    small[4]()
    out_ref[F:F + KP // 2, :] = ar2_fin[0]
    out_ref[F + KP // 2:F + KP, :] = ar2_fin[1]
    loss_row = out_ref[F + K:F + K + 1, :]
    out_ref[F + K:F + K + 1, :] = jnp.sum(loss_row, axis=1, keepdims=True) / label_count + jnp.zeros_like(loss_row)
    big[1]()
    drain1()
    drain2()
    big[2]()
    for between, when in ((True, is_mid), (False, mid == 0)):
        @pl.when(when)
        def _():
            for k, spec in enumerate(reduced[between]):
                reduce_copy(k, *spec).wait_send()
    for i in range(16):
        rcopy(outbox.at[i], pairin.at[i], rs_ps.at[i], rs_pr.at[i], pn).wait_send()
    big[3]()
    big[4]()
    out_ref[0:F // 2, :] = ar1_fin[0]
    out_ref[F // 2:F, :] = ar1_fin[1]


def unpack(packed, loss_out, dw1_out, dw2_out):
    loss_out[0] = packed[F + K, 0]
    dw1_out[...] = packed[0:F, :]
    dw2_out[...] = packed[F:F + K, :]


def solution(mesh):
    axis = 'nodes'

    def local_step(adj_rows, feat_rows, w_one, w_two, label_rows, mask_rows):
        rows = adj_rows.shape[0]
        dma = pltpu.SemaphoreType.DMA
        nsend = 144
        blk = lambda n: pltpu.VMEM((n, F, rows), F32)
        ar = lambda n: [pltpu.VMEM((2 * n, F), F32), pltpu.VMEM((n, F), F32), pltpu.VMEM((4, n, F), F32),
                        pltpu.VMEM((4, n, F), F32), pltpu.VMEM((2, n, F), F32)]
        vmem = pl.BlockSpec(memory_space=pltpu.VMEM)
        hbm = pl.BlockSpec(memory_space=pl.ANY)
        packed = pl.pallas_call(
            functools.partial(kernel, axis, rows),
            name='gcn_step',
            out_shape=pltpu.VMEM((F + KP, F), F32),
            in_specs=[hbm, hbm, vmem, vmem, vmem, vmem],
            out_specs=vmem,
            scratch_shapes=[
                pltpu.VMEM((NDEV, rows, rows), BF16), pltpu.VMEM((NDEV, rows + TAIL, F), BF16),
                pltpu.VMEM((NDEV, rows, F), BF16), pltpu.VMEM((rows, F), F32), pltpu.VMEM((rows, F), BF16),
                pltpu.VMEM((F, rows), BF16), pltpu.VMEM((F, rows), F32), pltpu.VMEM((F, F), F32),
                pltpu.VMEM((F, F), BF16), pltpu.VMEM((F, rows), BF16), pltpu.VMEM((TAIL, F), F32), pltpu.VMEM((TAIL, F), F32),
                pltpu.VMEM((rows, F), F32),
                blk(16), blk(16), blk(16), blk(6), blk(6), blk(6),
                pltpu.VMEM((4, 6, F - CUTS[-2], rows), F32),
                *ar(F // 2), *ar(KP // 2),
                dma((NDEV,)), dma(()), dma((NDEV, PIECES)), dma((nsend,)), dma((NDEV, PIECES)), dma((nsend,)),
                dma((16,)), dma((16,)), dma((64,)), dma((6, 3)), dma((6, 3)), dma((6, 3)), dma((4, 6)), dma((8,)), dma((10,)), dma((8,)), dma((10,)),
            ],
            compiler_params=pltpu.CompilerParams(collective_id=0, has_side_effects=True,
                                                 vmem_limit_bytes=60 * 1024 * 1024),
        )(adj_rows, feat_rows, w_one, w_two.T, label_rows.reshape(1, rows), mask_rows.reshape(rows // 128, 128))
        loss, dw_one, dw_two_t = pl.pallas_call(
            unpack,
            name='unpack',
            out_shape=(jax.ShapeDtypeStruct((1,), F32), jax.ShapeDtypeStruct((F, F), F32),
                       jax.ShapeDtypeStruct((K, F), F32)),
            in_specs=[vmem],
            out_specs=(pl.BlockSpec(memory_space=pltpu.SMEM), vmem, vmem),
        )(pltpu.with_memory_space_constraint(packed, pltpu.VMEM))
        return loss, dw_one, dw_two_t.T

    return jax.shard_map(local_step, mesh=mesh,
                         in_specs=(P(axis, None), P(axis, None), P(None, None), P(None, None), P(axis), P(axis)),
                         out_specs=(P(None), P(None, None), P(None, None)), check_vma=False)
```

```python
import functools

import jax
import jax.numpy as jnp
from jax import lax
from jax.experimental import pallas as pl
from jax.experimental.pallas import tpu as pltpu
from jax.sharding import PartitionSpec as P

MESH = pl.DeviceIdType.MESH
F32 = jnp.float32
BF16 = jnp.bfloat16
NDEV = 32
F = 128
K = 40
KP = 48
TAIL = 16

ORDER_END = (
    0, 16, 32, 1, 17, 40, 8, 2, 36, 5, 18, 21, 33, 44, 37, 24, 3, 12, 19, 34, 38, 10, 22, 28,
    29, 13, 26, 4, 7, 9, 6, 45, 23, 43, 41, 42, 11, 20, 39, 27, 25, 15, 30, 14, 46, 35, 47, 31,
)
ORDER_MID = (
    0, 16, 32, 2, 1, 18, 17, 36, 40, 3, 19, 10, 41, 26, 24, 34, 5, 38, 37, 42, 21, 44, 33, 4,
    43, 11, 20, 7, 45, 39, 8, 23, 9, 46, 27, 35, 22, 47, 14, 25, 30, 6, 15, 31, 13, 28, 29, 12,
)
PIECES = 3
BATCH = 4

CALC, DIAG, XSIDE, YSIDE, LINE, BACK, BDIAG, BX, BY, BEND = range(10)
CUTS = (0, 56, 104, 128)
REDUCE_END = (
    1, 83, 82, 367, 66, 366, 67, 2, 362, 210, 81, 363, 358, 131, 146, 211, 3, 147, 359, 195, 357, 354, 365, 65,
    194, 355, 130, 145, 364, 64, 361, 353, 259, 275, 209, 80, 416, 129, 193, 208, 274, 258, 128, 273, 352, 356, 144, 480,
    360, 192, 257, 544, 256, 272, 608,
)
REDUCE_MID = (
    1, 83, 67, 82, 64, 2, 147, 367, 65, 66, 366, 80, 362, 365, 211, 195, 363, 146, 81, 358, 359, 3, 354, 210,
    361, 131, 357, 364, 355, 416, 193, 360, 145, 353, 194, 129, 209, 259, 544, 356, 208, 130, 128, 275, 274, 352, 144, 192,
    480, 257, 273, 258, 272, 256, 608,
)


def program(order):
    seen, steps, ready, late, following = {}, [], [], [], []
    for code in order:
        c, q, j = code // 16, code // 4 % 4, code % 4
        steps.append((c, q, j))
        seen[q, j] = seen.get((q, j), 0) + 1
        if seen[q, j] == PIECES:
            ready.append((q, j))
            following.append((q, j))
            if len(ready) + len(late) >= BATCH:
                steps.append((ready, late))
                ready, late, following = [], following, []
    return steps + [(ready, late), ([], following)]


def kernel(axis, rows, a_hbm, x_hbm, w1_hbm, w2_hbm, lab_hbm, mask_hbm, out_ref,
           w1_v, lab_v, mask_v, p_sem,
           a_v, xall, hall, acc, s1, s1t, z1t, w2p, w2b, ut, mrow, cnt, sq,
           own, outbox, pairin, xin, yin, zin, zinb,
           ar1_src, ar1_pin, ar1_pl, ar1_zz, ar1_fin, ar2_src, ar2_pin, ar2_pl, ar2_zz, ar2_fin,
           a_sem, x_sem, ag1_r, ag1_s, ag2_r, ag2_s, rs_ps, rs_pr, rs_s, rs_xr, rs_yr, rs_zr, rs_br,
           ar1_s, ar1_r, ar2_s, ar2_r):
    me = lax.axis_index(axis)
    core = me % 2
    x = (me // 2) % 2
    y = (me // 4) % 2
    z = me // 8
    mid = ((z + 1) // 2) % 2
    half = z // 2
    z_in = 1 + z % 2
    z_out = (3 * z - 3) * mid + z * (1 - mid)

    def dev(xx, yy, zz, cc):
        return ((zz * 2 + yy) * 2 + xx) * 2 + cc

    xn, yn = dev(1 - x, y, z, core), dev(x, 1 - y, z, core)
    dn, pn = dev(1 - x, 1 - y, z, core), dev(x, y, z, 1 - core)
    zin_n, zout_n = dev(x, y, z_in, core), dev(x, y, z_out, core)
    zothers = [dev(x, y, (z + k) % 4, core) for k in (1, 2, 3)]

    def zk(j):
        late = j // 2
        line = late * j + (1 - late) * (j + mid * (1 - 2 * j))
        return line + half * (3 - 2 * line)

    def bid(q, j, other=0):
        qx, qy = q % 2, q // 2
        cc = core + other * (1 - 2 * core)
        return dev(x + qx * (1 - 2 * x), y + qy * (1 - 2 * y), zk(j), cc)

    def rcopy(src, dst, ssem, rsem, to):
        return pltpu.make_async_remote_copy(src_ref=src, dst_ref=dst, send_sem=ssem, recv_sem=rsem, device_id=(to,),
                                            device_id_type=MESH)

    def a_copy(b):
        cols = pl.ds(pl.multiple_of(b * rows, rows), rows)
        return pltpu.make_async_copy(a_hbm.at[:, cols], a_v.at[b], a_sem.at[b])

    x_copy = pltpu.make_async_copy(x_hbm, xall.at[me, pl.ds(0, rows)], x_sem)
    x_copy.start()
    mask_copy = pltpu.make_async_copy(mask_hbm, mask_v, p_sem.at[0])
    mask_copy.start()
    barrier = pltpu.get_barrier_semaphore()
    for to in [pn, xn, yn, dn] + zothers:
        pl.semaphore_signal(barrier, inc=1, device_id=(to,), device_id_type=MESH)
    blocks = {(q, j, o): bid(q, j, o) for q in range(4) for j in range(4) for o in range(2)}
    for b in blocks.values():
        a_copy(b).start()
    w1_copy = pltpu.make_async_copy(w1_hbm, w1_v, p_sem.at[1])
    w2_copy = pltpu.make_async_copy(w2_hbm, w2p.at[pl.ds(0, K)], p_sem.at[2])
    lab_copy = pltpu.make_async_copy(lab_hbm, lab_v, p_sem.at[3])
    for copy in (w1_copy, w2_copy, lab_copy):
        copy.start()
    mrow[...] = jnp.zeros_like(mrow)
    w2p[K:F, :] = jnp.zeros((F - K, F), F32)
    acc[...] = jnp.zeros_like(acc)
    mask_copy.wait()
    mrow[0:rows // 128, :] = mask_v[...].astype(F32)
    xall[me, rows:rows + TAIL, :] = mrow[...].astype(BF16)
    x_copy.wait()
    pl.semaphore_wait(barrier, 7)

    is_mid = mid == 1

    def pick(i, values):
        out = values[0]
        for k in range(1, len(values)):
            out = jnp.where(i == k, values[k], out)
        return out

    def gather(buf, cuts, r_sem, s_sem, first, between_sends=None):
        def piece(b, c):
            return buf.at[b, pl.ds(cuts[c], cuts[c + 1] - cuts[c])]

        def wait_recv(b, c):
            rcopy(piece(b, c), piece(b, c), s_sem.at[0], r_sem.at[b, c], pn).wait_recv()

        def targets(c, q, j, between):
            to = []
            if q == 0 or c == 2:
                if j == 0:
                    to += [zin_n, zout_n] if between else [zin_n]
                elif between:
                    to += [zin_n if j == 1 else zout_n]
            if q == 0 and (c < 2 or j == 0):
                to += [xn, yn]
            elif (q == 2 and c < 2 and j % 2 == 0) or (q == 2 and c == 2 and j == 0):
                to += [xn]
            elif q == 1 and c < 2 and j % 2 == 1:
                to += [yn]
            return to + [pn]

        def multiply(ready, late):
            ids = [blocks[q, j, 0] for q, j in ready] + [blocks[q, j, 1] for q, j in late]
            if not ids:
                return

            def body(i, carry):
                b = pick(i, ids)
                if late:
                    @pl.when(i >= len(ready))
                    def _():
                        for c in range(PIECES):
                            wait_recv(b, c)
                if first:
                    a_copy(b).wait()
                acc[...] += jnp.dot(a_v[b], buf[b, 0:rows, :], preferred_element_type=F32)
                return carry
            lax.fori_loop(0, len(ids), body, 0)

        def run(order, between, pending):
            own_left = PIECES
            for step in program(order):
                if len(step) == 2:
                    multiply(*step)
                    continue
                own_left -= step[1:] == (0, 0)
                if step[1:] != (0, 0) and own_left == 0:
                    own_left = -1
                    if between_sends is not None:
                        between_sends()
                c, q, j = step
                b = blocks[q, j, 0]
                if (q, j) != (0, 0):
                    wait_recv(b, c)
                for to in targets(c, q, j, between):
                    k = len(pending)
                    rcopy(piece(b, c), piece(b, c), s_sem.at[k], r_sem.at[b, c], to).start()
                    pending.append((b, c, to))

        sent = {True: [], False: []}

        @pl.when(is_mid)
        def _():
            run(ORDER_MID, True, sent[True])

        @pl.when(mid == 0)
        def _():
            run(ORDER_END, False, sent[False])

        def drain():
            for between, when in ((True, is_mid), (False, mid == 0)):
                @pl.when(when)
                def _():
                    for k, (b, c, to) in enumerate(sent[between]):
                        rcopy(piece(b, c), piece(b, c), s_sem.at[k], r_sem.at[b, c], to).wait_send()
        return drain

    cuts1 = (0, rows * 3 // 8, rows * 6 // 8, rows + TAIL)
    cuts2 = (0, rows * 3 // 8, rows * 6 // 8, rows)
    drain1 = gather(xall, cuts1, ag1_r, ag1_s, True)

    s1b = acc[...].astype(BF16)
    s1[...] = s1b
    w1_copy.wait()
    z1 = jnp.dot(s1b, w1_v[...].astype(BF16), preferred_element_type=F32)
    hall[me] = jnp.maximum(z1, 0.0).astype(BF16)
    sq[...] = z1
    acc[...] = jnp.zeros_like(acc)

    def count_body(b, tot):
        return tot + xall[b, rows:rows + TAIL, :].astype(F32)

    def early():
        w2b[...] = w2p[...].T.astype(BF16)
        z1t[...] = sq[...].T
        s1t[...] = s1[...].astype(F32).T.astype(BF16)
        cnt[...] = lax.fori_loop(0, NDEV, count_body, jnp.zeros((TAIL, 128), F32))

    w2_copy.wait()
    lab_copy.wait()
    drain2 = gather(hall, cuts2, ag2_r, ag2_s, False, early)

    w2t = w2p[0:KP, :].astype(BF16)
    label_count = jnp.sum(cnt[...])
    s2b = acc[...].astype(BF16)
    z2 = lax.dot_general(w2t, s2b, (((1,), (1,)), ((), ())), preferred_element_type=F32)
    row_id = lax.broadcasted_iota(jnp.int32, (KP, rows), 0)
    valid = row_id < K
    top = jnp.max(jnp.where(valid, z2, -jnp.inf), axis=0, keepdims=True)
    shifted = jnp.where(valid, z2 - top, 0.0)
    norm = jnp.log(jnp.sum(jnp.where(valid, jnp.exp(shifted), 0.0), axis=0, keepdims=True))
    log_prob = shifted - norm
    hot = row_id == lab_v[...]
    onehot = jnp.where(hot, 1.0, 0.0)
    weight = jnp.concatenate([mrow[k:k + 1, :] for k in range(rows // 128)], axis=1)
    loss_row = -weight * jnp.sum(jnp.where(hot, log_prob, 0.0), axis=0, keepdims=True)
    g2 = jnp.where(valid, weight * (jnp.exp(log_prob) - onehot) / label_count, 0.0).astype(BF16)
    ut[...] = jnp.dot(w2b[:, 0:KP], g2, preferred_element_type=F32).astype(BF16)
    dw2t = jnp.dot(g2, s2b, preferred_element_type=F32)
    loss_part = loss_row[:, 0:128]
    for k in range(1, rows // 128):
        loss_part = loss_part + loss_row[:, k * 128:(k + 1) * 128]
    ar2_src[...] = dw2t
    ar2_src[K:K + 1, :] = loss_part

    plane = y * 2 + x

    def make_ar(src, pin, pl4, zz, fin, s_sem, r_sem):
        n = src.shape[0] // 2

        def give():
            lo = pl.multiple_of((1 - core) * n, n)
            return [rcopy(src.at[pl.ds(lo, n)], pin, s_sem.at[0], r_sem.at[0], pn)]

        def over_plane():
            return [rcopy(pl4.at[plane], pl4.at[plane], s_sem.at[1 + k], r_sem.at[1 + plane], to)
                    for k, to in enumerate((xn, yn, dn))]

        def over_line():
            return [rcopy(zz.at[z], zz.at[z], s_sem.at[4 + k], r_sem.at[5 + z], to) for k, to in enumerate(zothers)]

        def back():
            return [rcopy(fin.at[core], fin.at[core], s_sem.at[7], r_sem.at[9], pn)]

        def start(copies):
            for c in copies:
                c.start()

        def s1():
            start(give())

        def s2():
            rcopy(pin, pin, s_sem.at[0], r_sem.at[0], pn).wait_recv()
            lo = pl.multiple_of(core * n, n)
            pl4[plane] = src[pl.ds(lo, n), :] + pin[...]
            start(over_plane())

        def s3():
            for px, py in ((1, 0), (0, 1), (1, 1)):
                p = (y + py * (1 - 2 * y)) * 2 + x + px * (1 - 2 * x)
                rcopy(pl4.at[p], pl4.at[p], s_sem.at[0], r_sem.at[1 + p], pn).wait_recv()
            zz[z] = (pl4[0] + pl4[1]) + (pl4[2] + pl4[3])
            start(over_line())

        def s4():
            for k in (1, 2, 3):
                o = (z + k) % 4
                rcopy(zz.at[o], zz.at[o], s_sem.at[0], r_sem.at[5 + o], pn).wait_recv()
            fin[core] = (zz[0] + zz[1]) + (zz[2] + zz[3])
            start(back())

        def s5():
            rcopy(fin.at[1 - core], fin.at[1 - core], s_sem.at[0], r_sem.at[9], pn).wait_recv()
            for c in give() + over_plane() + over_line() + back():
                c.wait_send()

        return s1, s2, s3, s4, s5

    small = make_ar(ar2_src, ar2_pin, ar2_pl, ar2_zz, ar2_fin, ar2_s, ar2_r)
    small[0]()

    def parts(q, j):
        i = q * 4 + j
        outbox[i] = jnp.dot(ut[...], a_v[bid(q, j, 1)], preferred_element_type=F32)
        rcopy(outbox.at[i], pairin.at[i], rs_ps.at[i], rs_pr.at[i], pn).start()
        own[i] = jnp.dot(ut[...], a_v[bid(q, j)], preferred_element_type=F32)

    def diag_body(k, carry):
        parts(3, 3 - k)
        return carry

    def side_body(k, carry):
        parts(1 + k % 2, 3 - k // 2)
        return carry

    def own_body(k, carry):
        parts(0, 3 - k)
        return carry

    def piece_rows(c):
        return pl.ds(CUTS[c], CUTS[c + 1] - CUTS[c])

    def landed(ref, sem):
        rcopy(ref, ref, rs_s.at[0], sem, pn).wait_recv()

    to_line = zin_n + mid * (zout_n - zin_n)
    mid_slot = {3: 3, 2: 2, 1: 5, 0: 0}
    line_slot = {3: 3 + 2 * mid, 2: 2 + 2 * mid, 1: 4 * mid}
    line_to = {3: zin_n, 2: zin_n, 1: to_line}

    def reduce_copy(k, i, c, dst, slot, r_sem, r_slot, to):
        target = dst.at[slot] if dst is zinb else dst.at[slot, piece_rows(c)]
        return rcopy(own.at[i, piece_rows(c)], target, rs_s.at[k], r_sem.at[r_slot], to)

    def reduce(order, between, sent):
        added = set()

        def value(q, j):
            i = q * 4 + j
            if i not in added:
                added.add(i)
                rcopy(pairin.at[i], pairin.at[i], rs_ps.at[0], rs_pr.at[i], pn).wait_recv()
                own[i] = own[i] + pairin[i]
            return i

        def send(i, dst, slot, r_sem, r_slot, to):
            sent.append((i, c, dst, slot, r_sem, r_slot, to))
            reduce_copy(len(sent) - 1, *sent[-1]).start()

        for code in order:
            kind, c, q, j = code // 64, code // 16 % 4, code // 4 % 4, code % 4
            if kind == CALC:
                if j == 1:
                    lax.fori_loop(0, 4, diag_body, 0)
                elif j == 2:
                    lax.fori_loop(0, 8, side_body, 0)
                    small[1]()
                else:
                    lax.fori_loop(0, 4, own_body, 0)
                continue
            hs = piece_rows(c)
            diag = (3 - j) // 2
            if kind == DIAG:
                i = value(3, j)
                if j % 2 == 1:
                    send(i, xin, diag, rs_xr, (diag, c), xn)
                else:
                    send(i, yin, diag, rs_yr, (diag, c), yn)
            elif kind == XSIDE:
                i = value(1, j)
                if j % 2 == 0:
                    landed(yin.at[diag, hs], rs_yr.at[diag, c])
                    own[i, hs] = own[i, hs] + yin[diag, hs]
                send(i, xin, 2 + j, rs_xr, (2 + j, c), xn)
            elif kind == YSIDE:
                i = value(2, j)
                if j % 2 == 1:
                    landed(xin.at[diag, hs], rs_xr.at[diag, c])
                    own[i, hs] = own[i, hs] + xin[diag, hs]
                send(i, yin, 2 + j, rs_yr, (2 + j, c), yn)
            elif kind == LINE:
                i = value(0, j)
                landed(xin.at[2 + j, hs], rs_xr.at[2 + j, c])
                landed(yin.at[2 + j, hs], rs_yr.at[2 + j, c])
                own[i, hs] = (own[i, hs] + xin[2 + j, hs]) + yin[2 + j, hs]
                for t in ([mid_slot[j]] if between else []) + ([4] if j == 0 else []):
                    landed(zin.at[t, hs], rs_zr.at[t, c])
                    own[i, hs] = own[i, hs] + zin[t, hs]
                if j > 0:
                    send(i, zin, line_slot[j], rs_zr, (line_slot[j], c), line_to[j])
            elif kind == BACK:
                i = value(q, j)
                for t in ([mid_slot[j]] if between else []) + ([4] if j == 0 else []):
                    landed(zinb.at[q, t], rs_br.at[q, t])
                    own[i, hs] = own[i, hs] + zinb[q, t]
                if j > 0:
                    send(i, zinb, (q, line_slot[j]), rs_br, (q, line_slot[j]), line_to[j])
            elif kind == BDIAG:
                send(12, xin, 0, rs_xr, (0, c), xn)
            elif kind == BX:
                send(4, xin, 2, rs_xr, (2, c), xn)
            elif kind == BY:
                landed(xin.at[0, hs], rs_xr.at[0, c])
                own[8, hs] = own[8, hs] + xin[0, hs]
                send(8, yin, 2, rs_yr, (2, c), yn)
            else:
                landed(xin.at[2, hs], rs_xr.at[2, c])
                landed(yin.at[2, hs], rs_yr.at[2, c])
                own[0, hs] = (own[0, hs] + xin[2, hs]) + yin[2, hs]
            steps_left = len(order) - 1 - order.index(code)
            if steps_left == 24:
                small[2]()
            elif steps_left == 6:
                small[3]()

    reduced = {True: [], False: []}

    @pl.when(is_mid)
    def _():
        reduce(REDUCE_MID, True, reduced[True])

    @pl.when(mid == 0)
    def _():
        reduce(REDUCE_END, False, reduced[False])

    g1t = jnp.where(z1t[...] > 0.0, own[0], 0.0).astype(BF16)
    ar1_src[...] = lax.dot_general(s1t[...], g1t, (((1,), (1,)), ((), ())), preferred_element_type=F32)
    big = make_ar(ar1_src, ar1_pin, ar1_pl, ar1_zz, ar1_fin, ar1_s, ar1_r)
    big[0]()
    small[4]()
    out_ref[F:F + KP // 2, :] = ar2_fin[0]
    out_ref[F + KP // 2:F + KP, :] = ar2_fin[1]
    loss_row = out_ref[F + K:F + K + 1, :]
    out_ref[F + K:F + K + 1, :] = jnp.sum(loss_row, axis=1, keepdims=True) / label_count + jnp.zeros_like(loss_row)
    big[1]()
    drain1()
    drain2()
    big[2]()
    for between, when in ((True, is_mid), (False, mid == 0)):
        @pl.when(when)
        def _():
            for k, spec in enumerate(reduced[between]):
                reduce_copy(k, *spec).wait_send()
    for i in range(16):
        rcopy(outbox.at[i], pairin.at[i], rs_ps.at[i], rs_pr.at[i], pn).wait_send()
    big[3]()
    big[4]()
    out_ref[0:F // 2, :] = ar1_fin[0]
    out_ref[F // 2:F, :] = ar1_fin[1]


def unpack(packed, loss_out, dw1_out, dw2_out):
    loss_out[0] = packed[F + K, 0]
    dw1_out[...] = packed[0:F, :]
    dw2_out[...] = packed[F:F + K, :]


def solution(mesh):
    axis = 'nodes'

    def local_step(adj_rows, feat_rows, w_one, w_two, label_rows, mask_rows):
        rows = adj_rows.shape[0]
        dma = pltpu.SemaphoreType.DMA
        nsend = 144
        blk = lambda n: pltpu.VMEM((n, F, rows), F32)
        ar = lambda n: [pltpu.VMEM((2 * n, F), F32), pltpu.VMEM((n, F), F32), pltpu.VMEM((4, n, F), F32),
                        pltpu.VMEM((4, n, F), F32), pltpu.VMEM((2, n, F), F32)]
        vmem = pl.BlockSpec(memory_space=pltpu.VMEM)
        hbm = pl.BlockSpec(memory_space=pltpu.HBM)
        packed = pl.pallas_call(
            functools.partial(kernel, axis, rows),
            name='gcn_step',
            out_shape=pltpu.VMEM((F + KP, F), F32),
            in_specs=[hbm] * 6,
            out_specs=vmem,
            scratch_shapes=[
                pltpu.VMEM((F, F), F32), pltpu.VMEM((1, rows), jnp.int32), pltpu.VMEM((rows // 128, 128), jnp.int32),
                dma((4,)),
                pltpu.VMEM((NDEV, rows, rows), BF16), pltpu.VMEM((NDEV, rows + TAIL, F), BF16),
                pltpu.VMEM((NDEV, rows, F), BF16), pltpu.VMEM((rows, F), F32), pltpu.VMEM((rows, F), BF16),
                pltpu.VMEM((F, rows), BF16), pltpu.VMEM((F, rows), F32), pltpu.VMEM((F, F), F32),
                pltpu.VMEM((F, F), BF16), pltpu.VMEM((F, rows), BF16), pltpu.VMEM((TAIL, F), F32), pltpu.VMEM((TAIL, F), F32),
                pltpu.VMEM((rows, F), F32),
                blk(16), blk(16), blk(16), blk(6), blk(6), blk(6),
                pltpu.VMEM((4, 6, F - CUTS[-2], rows), F32),
                *ar(F // 2), *ar(KP // 2),
                dma((NDEV,)), dma(()), dma((NDEV, PIECES)), dma((nsend,)), dma((NDEV, PIECES)), dma((nsend,)),
                dma((16,)), dma((16,)), dma((64,)), dma((6, 3)), dma((6, 3)), dma((6, 3)), dma((4, 6)), dma((8,)), dma((10,)), dma((8,)), dma((10,)),
            ],
            compiler_params=pltpu.CompilerParams(collective_id=0, has_side_effects=True,
                                                 vmem_limit_bytes=60 * 1024 * 1024),
        )(adj_rows, feat_rows, w_one, w_two.T, label_rows.reshape(1, rows), mask_rows.reshape(rows // 128, 128))
        loss, dw_one, dw_two_t = pl.pallas_call(
            unpack,
            name='unpack',
            out_shape=(jax.ShapeDtypeStruct((1,), F32), jax.ShapeDtypeStruct((F, F), F32),
                       jax.ShapeDtypeStruct((K, F), F32)),
            in_specs=[vmem],
            out_specs=(pl.BlockSpec(memory_space=pltpu.SMEM), vmem, vmem),
        )(pltpu.with_memory_space_constraint(packed, pltpu.VMEM))
        return loss, dw_one, dw_two_t.T

    return jax.shard_map(local_step, mesh=mesh,
                         in_specs=(P(axis, None), P(axis, None), P(None, None), P(None, None), P(axis), P(axis)),
                         out_specs=(P(None), P(None, None), P(None, None)), check_vma=False)
```
